256 devices in a mesh: groups: 2 (over z), patch: 128 (over x, y, core).
Axes of the slice: x: 8, y: 8, z: 2, core: 2. Of those that a mesh axis runs over, the one named last changes fastest.
The devices are a block of a 8x8x16 slice.
Arguments:
- nodes: bfloat16 [81920, 512], P(('groups', 'patch')), parts along dimension 0, may hold values from -6 to 6
- edges: bfloat16 [393216, 512], P(('groups', 'patch')), parts along dimension 0, may hold values from -6 to 6
- node_cot: bfloat16 [81920, 512], P(('groups', 'patch')), parts along dimension 0, may hold values from -6 to 6
- edge_cot: bfloat16 [393216, 512], P(('groups', 'patch')), parts along dimension 0, may hold values from -6 to 6
- w_edge: bfloat16 [512, 512], replicated, may hold values from -0.15625 to 0.15625
- w_send: bfloat16 [512, 512], replicated, may hold values from -0.15625 to 0.15625
- w_recv: bfloat16 [512, 512], replicated, may hold values from -0.15625 to 0.15625
- edge_bias: float32 [512], replicated, may hold values from -3 to 3
- w_edge_out: bfloat16 [512, 512], replicated, may hold values from -0.25 to 0.25
- edge_out_bias: float32 [512], replicated, may hold values from -3 to 3
- edge_gain: float32 [512], replicated, may hold values from 0.25 to 1.75
- w_node: bfloat16 [512, 512], replicated, may hold values from -0.1875 to 0.1875
- w_agg: bfloat16 [512, 512], replicated, may hold values from -0.1875 to 0.1875
- node_bias: float32 [512], replicated, may hold values from -3 to 3
- w_node_out: bfloat16 [512, 512], replicated, may hold values from -0.25 to 0.25
- node_out_bias: float32 [512], replicated, may hold values from -3 to 3
- node_gain: float32 [512], replicated, may hold values from 0.25 to 1.75
- send_slots: int32 [196608], P('patch'), may hold values from 0 to 831, as said below
- recv_slots: int32 [196608], P('patch'), may hold values from 0 to 319
- neighbour_send_lists: int32 [512, 64], P('patch'), may hold values from 0 to 319
- coarse_rows: int32 [1024], P('patch'), may hold values from 0 to 319, as said below
- far_lists: int32 [128, 128, 2], P('patch'), may hold values from 0 to 7
- block_count: int32 [128], P('patch'), may hold values from 6 to 12, as said below
Outputs:
- new_nodes: bfloat16 [81920, 512], P(('groups', 'patch')), parts along dimension 0
- new_edges: bfloat16 [393216, 512], P(('groups', 'patch')), parts along dimension 0
- node_grad: bfloat16 [81920, 512], P(('groups', 'patch')), parts along dimension 0
- edge_grad: bfloat16 [393216, 512], P(('groups', 'patch')), parts along dimension 0
The draws below stay inside these ranges and needn't reach their ends.
There are 2 independent parts, one for each index of `groups`. The reference program is written for one: setup_inputs(seed, part) draws one part's arguments, and reference() takes and returns one part's arrays. A program takes and returns all parts, laid end to end along the dimension named above; an argument that names none is the same for every part. Nothing has to cross between parts.
Inputs may be any that keep to these rules, and one draw needn't show every extreme that they name: `send_slots`: addresses below 320 are rows of the edge's own patch, the next 256 are neighbour slots, the last 128 * 2 are distant slots. `coarse_rows`: the 8 rows of one patch are distinct. `block_count`: some patches have all 12 blocks live in every draw.
All inputs are finite; a program needn't handle non-finite values.
Results may differ from the reference program's by a relative error of at most 0.013.
Values may be sent and summed in bfloat16 or wider, within the bound.
A program may use at most 128 MiB of HBM per device.

```python
import jax
import jax.numpy as jnp
from jax import lax

D = 512
HID = 512
PATCH_NODES = 320
EDGE_BLOCKS = 12
BLOCK = 128
NEIGHBOUR_COUNT = 4
NEAR_SLOT_ROWS = 64
FAR_SLOT_ROWS = 2
COARSE_DEV = 8
NODES = 40960
EDGES_DEV = 1536
EDGE_SLOTS_ALL = 196608
N_PATCH = 128


def draw_send_slots(key, part):
    random_keys = jax.random.split(jax.random.fold_in(key, 11), 4)
    kind = jax.random.randint(random_keys[0], (EDGE_SLOTS_ALL,), 0, 20)
    local_rows = jax.random.randint(random_keys[1], (EDGE_SLOTS_ALL,), 0, PATCH_NODES)
    neighbour_rows = PATCH_NODES + jax.random.randint(random_keys[2], (EDGE_SLOTS_ALL,), 0, NEIGHBOUR_COUNT * NEAR_SLOT_ROWS)
    distant_rows = PATCH_NODES + NEIGHBOUR_COUNT * NEAR_SLOT_ROWS + jax.random.randint(random_keys[3], (EDGE_SLOTS_ALL,), 0, N_PATCH * FAR_SLOT_ROWS)
    return jnp.where(kind < 12, local_rows, jnp.where(kind < 17, neighbour_rows, distant_rows)).astype(jnp.int32)


def draw_coarse_rows(key, part):
    random_keys = jax.random.split(jax.random.fold_in(key, 23), N_PATCH)

    def choose(single):
        return jax.random.permutation(single, PATCH_NODES)[:COARSE_DEV]
    return jax.vmap(choose)(random_keys).reshape(-1).astype(jnp.int32)


def draw_block_count(key, part):
    random_keys = jax.random.split(jax.random.fold_in(key, 37), 2)
    lowest = max(1, EDGE_BLOCKS // 2)
    counts = jax.random.randint(random_keys[0], (N_PATCH,), lowest, EDGE_BLOCKS + 1)
    busiest = jax.random.permutation(random_keys[1], N_PATCH)[:3]
    return counts.at[busiest].set(EDGE_BLOCKS).astype(jnp.int32)


def place_ends(drawn, stream_key, low, top_value):
    shape = drawn.shape
    place = [jax.random.randint(jax.random.fold_in(stream_key, axis), (), 0, shape[axis]) for axis in range(len(shape))]
    drawn = drawn.at[tuple(place)].set(low)
    longest = shape.index(max(shape))
    place[longest] = (place[longest] + 1) % shape[longest]
    return drawn.at[tuple(place)].set(top_value)


def steps_of(stream_key, extent, shards, low, high):
    level = 1.0
    for dim, parts in shards:
        heights = jax.random.uniform(jax.random.fold_in(jax.random.fold_in(stream_key, 6), dim), (parts,), jnp.float32, low / len(shards), high / len(shards))
        level = level * jnp.repeat(jnp.exp(heights), extent[dim] // parts).reshape((-1,) + (1,) * (len(extent) - 1 - dim))
    return level


def gaussian(stream_key, dims, scale, bound, cuts=(), kind=jnp.bfloat16):
    values = scale * jax.random.normal(stream_key, dims, jnp.float32)
    if cuts:
        values = values * steps_of(stream_key, dims, cuts, -0.22, 0.18)
    return jnp.clip(values, -bound, bound).astype(kind)


def setup_inputs(seed: int = 0, part: int = 0) -> dict:
    keys = jax.random.split(jax.random.key(seed), 24)
    own_keys = jax.random.split(jax.random.fold_in(keys[23], part), 24)
    nodes = gaussian(own_keys[0], (NODES, D), 1.0, 6.0, ((0, 128),))
    edges = gaussian(own_keys[1], (EDGE_SLOTS_ALL, D), 1.0, 6.0, ((0, 128),))
    node_cot = gaussian(own_keys[2], (NODES, D), 1.0, 6.0, ((0, 128),))
    edge_cot = gaussian(own_keys[3], (EDGE_SLOTS_ALL, D), 1.0, 6.0, ((0, 128),))
    w_edge = gaussian(keys[4], (D, HID), (3 * D) ** -0.5, 0.15625)
    w_send = gaussian(keys[5], (D, HID), (3 * D) ** -0.5, 0.15625)
    w_recv = gaussian(keys[6], (D, HID), (3 * D) ** -0.5, 0.15625)
    edge_bias = gaussian(keys[7], (HID,), 0.5, 3.0, (), jnp.float32)
    w_edge_out = gaussian(keys[8], (HID, D), HID ** -0.5, 0.25)
    edge_out_bias = gaussian(keys[9], (D,), 0.5, 3.0, (), jnp.float32)
    edge_gain = jnp.clip(1.0 + 0.15 * jax.random.normal(keys[10], (D,), jnp.float32), 0.25, 1.75)
    w_node = gaussian(keys[11], (D, HID), (2 * D) ** -0.5, 0.1875)
    w_agg = gaussian(keys[12], (D, HID), (2 * D) ** -0.5, 0.1875)
    node_bias = gaussian(keys[13], (HID,), 0.5, 3.0, (), jnp.float32)
    w_node_out = gaussian(keys[14], (HID, D), HID ** -0.5, 0.25)
    node_out_bias = gaussian(keys[15], (D,), 0.5, 3.0, (), jnp.float32)
    node_gain = jnp.clip(1.0 + 0.15 * jax.random.normal(keys[16], (D,), jnp.float32), 0.25, 1.75)
    send_slots = draw_send_slots(jax.random.fold_in(keys[23], 71), part)
    recv_slots = place_ends(jax.random.randint(keys[18], (EDGE_SLOTS_ALL,), 0, PATCH_NODES), jax.random.fold_in(keys[18], 1), 0, PATCH_NODES - 1).astype(jnp.int32)
    neighbour_send_lists = place_ends(jax.random.randint(keys[19], (N_PATCH * NEIGHBOUR_COUNT, NEAR_SLOT_ROWS), 0, PATCH_NODES), jax.random.fold_in(keys[19], 1), 0, PATCH_NODES - 1).astype(jnp.int32)
    coarse_rows = draw_coarse_rows(jax.random.fold_in(keys[23], 71), part)
    far_lists = place_ends(jax.random.randint(keys[21], (N_PATCH, N_PATCH, FAR_SLOT_ROWS), 0, COARSE_DEV), jax.random.fold_in(keys[21], 1), 0, COARSE_DEV - 1).astype(jnp.int32)
    block_count = draw_block_count(jax.random.fold_in(keys[23], 71), part)
    return dict(nodes=nodes, edges=edges, node_cot=node_cot, edge_cot=edge_cot, w_edge=w_edge, w_send=w_send, w_recv=w_recv, edge_bias=edge_bias, w_edge_out=w_edge_out, edge_out_bias=edge_out_bias, edge_gain=edge_gain, w_node=w_node, w_agg=w_agg, node_bias=node_bias, w_node_out=w_node_out, node_out_bias=node_out_bias, node_gain=node_gain, send_slots=send_slots, recv_slots=recv_slots, neighbour_send_lists=neighbour_send_lists, coarse_rows=coarse_rows, far_lists=far_lists, block_count=block_count)


def normalize(values):
    center = values - lax.optimization_barrier(jnp.mean(values, axis=-1, keepdims=True))
    spread = lax.optimization_barrier(jnp.mean(center * center, axis=-1, keepdims=True))
    return center * lax.rsqrt(spread + 1e-05)

def layer(node_rows, edge_rows, table, sending_patch, receiver, live, params):
    w_edge, w_send, w_recv, edge_bias, w_edge_out, edge_out_bias, edge_gain, w_node, w_agg, node_bias, w_node_out, node_out_bias, node_gain = params
    send_rows = jnp.take(table, sending_patch, axis=0).astype(jnp.bfloat16)
    recv_rows = jnp.take(node_rows, receiver, axis=0).astype(jnp.bfloat16)
    pre_edge = jnp.dot(edge_rows.astype(jnp.bfloat16), w_edge, preferred_element_type=jnp.float32)
    pre_edge = pre_edge + jnp.dot(send_rows, w_send, preferred_element_type=jnp.float32)
    pre_edge = pre_edge + jnp.dot(recv_rows, w_recv, preferred_element_type=jnp.float32) + edge_bias
    edge_hidden = jax.nn.silu(pre_edge).astype(jnp.bfloat16)
    edge_out = jnp.dot(edge_hidden, w_edge_out, preferred_element_type=jnp.float32) + edge_out_bias
    message = live[:, None] * edge_gain * normalize(edge_out)
    new_edges = edge_rows + message
    sent_message = message.astype(jnp.bfloat16)
    aggregate = jax.ops.segment_sum(sent_message.astype(jnp.float32), receiver, num_segments=node_rows.shape[0])
    aggregate = aggregate.astype(jnp.bfloat16)
    pre_node = jnp.dot(node_rows.astype(jnp.bfloat16), w_node, preferred_element_type=jnp.float32)
    pre_node = pre_node + jnp.dot(aggregate, w_agg, preferred_element_type=jnp.float32) + node_bias
    node_hidden = jax.nn.silu(pre_node).astype(jnp.bfloat16)
    node_out = jnp.dot(node_hidden, w_node_out, preferred_element_type=jnp.float32) + node_out_bias
    new_nodes = node_rows + node_gain * normalize(node_out)
    return (new_nodes, new_edges)

def reference(nodes, edges, node_cot, edge_cot, w_edge, w_send, w_recv, edge_bias, w_edge_out, edge_out_bias, edge_gain, w_node, w_agg, node_bias, w_node_out, node_out_bias, node_gain, send_slots, recv_slots, neighbour_send_lists, coarse_rows, far_lists, block_count):
    params = (w_edge, w_send, w_recv, edge_bias, w_edge_out, edge_out_bias, edge_gain, w_node, w_agg, node_bias, w_node_out, node_out_bias, node_gain)
    patch_count_total = N_PATCH
    position = jnp.arange(EDGE_SLOTS_ALL, dtype=jnp.int32)
    owner = position // EDGES_DEV
    row_address = send_slots
    home_node = owner * PATCH_NODES + row_address
    neighbour_patch = jnp.clip(row_address - PATCH_NODES, 0, NEIGHBOUR_COUNT * NEAR_SLOT_ROWS - 1)
    neighbour_offset = neighbour_patch // NEAR_SLOT_ROWS
    neighbour_slot = neighbour_patch % NEAR_SLOT_ROWS
    offset = (neighbour_offset // 2 + 1) * (1 - 2 * (neighbour_offset % 2))
    near_source = (owner - offset) % patch_count_total
    neighbour_node = near_source * PATCH_NODES + neighbour_send_lists[near_source * NEIGHBOUR_COUNT + neighbour_offset, neighbour_slot]
    distant_patch = jnp.clip(row_address - PATCH_NODES - NEIGHBOUR_COUNT * NEAR_SLOT_ROWS, 0, patch_count_total * FAR_SLOT_ROWS - 1)
    far_source = distant_patch // FAR_SLOT_ROWS
    far_slot = distant_patch % FAR_SLOT_ROWS
    coarse_index = far_lists[owner, far_source, far_slot]
    distant_node = far_source * PATCH_NODES + coarse_rows[far_source * COARSE_DEV + coarse_index]
    sending_patch = jnp.where(row_address < PATCH_NODES, home_node, jnp.where(row_address < PATCH_NODES + NEIGHBOUR_COUNT * NEAR_SLOT_ROWS, neighbour_node, distant_node)).astype(jnp.int32)
    receiver = (owner * PATCH_NODES + recv_slots).astype(jnp.int32)
    live = (position % EDGES_DEV // BLOCK < block_count[owner]).astype(jnp.float32)
    nodes_wide = nodes.astype(jnp.float32)
    edges_wide = edges.astype(jnp.float32)

    def forward(node_rows, edge_rows):
        return layer(node_rows, edge_rows, node_rows, sending_patch, receiver, live, params)
    (new_nodes, new_edges), pull = jax.vjp(forward, nodes_wide, edges_wide)
    node_grad, edge_grad = pull((node_cot.astype(jnp.float32), edge_cot.astype(jnp.float32)))
    return (new_nodes.astype(jnp.bfloat16), new_edges.astype(jnp.bfloat16), node_grad.astype(jnp.bfloat16), edge_grad.astype(jnp.bfloat16))
```

```python
import functools

import jax
import jax.numpy as jnp
from jax import lax
from jax.experimental import pallas as pl
from jax.experimental.pallas import tpu as pltpu
from jax.sharding import PartitionSpec as P

BLOCK = 128
LANES = 128
MESH = pl.DeviceIdType.MESH
F32 = jnp.float32
BF16 = jnp.bfloat16
STRIDE = 75


def mm(a, b):
    return lax.dot_general(a, b, (((1,), (0,)), ((), ())), preferred_element_type=F32)


def mm_nt(a, b):
    return lax.dot_general(a, b, (((1,), (1,)), ((), ())), preferred_element_type=F32)


def mm_tn(a, b):
    return lax.dot_general(a, b, (((0,), (0,)), ((), ())), preferred_element_type=F32)


def iota(shape, dim):
    return lax.broadcasted_iota(jnp.int32, shape, dim)


def hot(mask):
    return jnp.where(mask, 1.0, 0.0).astype(BF16)


def offsets_of(count):
    return [(index // 2 + 1) * (1 - 2 * (index % 2)) for index in range(count)]


def peers_loop(peers, body):
    me = lax.axis_index("patch")

    def step(i, carry):
        body(lax.rem(me + lax.rem(i * STRIDE, peers), peers))
        return carry

    lax.fori_loop(1, peers, step, 0)


def greet_all(peers):
    barrier = pltpu.get_barrier_semaphore()

    def greet(peer):
        pl.semaphore_signal(barrier, inc=1, device_id={"patch": peer}, device_id_type=MESH)

    peers_loop(peers, greet)
    return barrier


def remote(src, dst, send, recv, peer):
    return pltpu.make_async_remote_copy(
        src_ref=src, dst_ref=dst, send_sem=send, recv_sem=recv,
        device_id={"patch": peer}, device_id_type=MESH,
    )


def spread_rows(pair, wide, packed, peers):
    parts = pair[0].shape[1] // LANES
    unit = 2 * parts
    for slot in range(2):
        for part in range(parts):
            wide[pl.ds(2 * part + slot, peers, stride=unit), :] = pair[slot][
                :, part * LANES : (part + 1) * LANES
            ]
    packed[...] = wide[...].reshape(peers, unit, LANES).astype(BF16)


def collect_rows(packed, wide, peers, width):
    parts = width // LANES
    unit = 2 * parts
    wide[...] = packed[...].astype(F32).reshape(peers * unit, LANES)
    pair = []
    for slot in range(2):
        pieces = [
            wide[pl.ds(2 * part + slot, peers, stride=unit), :] for part in range(parts)
        ]
        pair.append(jnp.concatenate(pieces, axis=1))
    return pair


def send_kernel(
    peers, nodes, near_lists, far_lists, coarse,
    table, coarse_slots,
    near_out, near_in, idx_out, idx_in, wide, far_out, far_in,
    near_send, near_recv, sems,
):
    me = lax.axis_index("patch")
    own, width = nodes.shape
    near_count, near_rows = near_lists.shape
    barrier = greet_all(peers)

    for k in range(near_count):
        mask = iota((own, near_rows), 0) == near_lists[k : k + 1, :]
        near_out[k] = mm_tn(hot(mask), nodes[...]).astype(BF16)
    wanted = far_lists[0]
    lane = iota((peers, LANES), 1)
    idx_out[...] = jnp.where(lane == 0, wanted[:, 0:1], wanted[:, 1:2]).reshape(peers, 1, LANES)

    pl.semaphore_wait(barrier, peers - 1)
    offsets = offsets_of(near_count)
    near = []
    for k in range(near_count):
        copy = remote(
            near_out.at[k], near_in.at[k], near_send.at[k], near_recv.at[k],
            lax.rem(me + offsets[k] + peers, peers),
        )
        copy.start()
        near.append(copy)
    peers_loop(
        peers,
        lambda peer: remote(
            idx_out.at[peer], idx_in.at[me], sems.at[0], sems.at[1], peer
        ).start(),
    )
    idx_in[pl.ds(me, 1)] = idx_out[pl.ds(me, 1)]
    others = pl.ds(0, peers - 1)
    remote(idx_out.at[others], idx_in.at[others], sems.at[0], sems.at[1], me).wait_recv()

    asked = idx_in[...].reshape(peers, LANES)
    slots = jnp.zeros_like(asked)
    for c in range(coarse.shape[0]):
        slots = jnp.where(asked == c, coarse[c], slots)
    coarse_slots[...] = slots
    pair = [mm(hot(iota((peers, own), 1) == slots[:, s : s + 1]), nodes[...]) for s in range(2)]
    spread_rows(pair, wide, far_out, peers)
    peers_loop(
        peers,
        lambda peer: remote(
            far_out.at[peer], far_in.at[me], sems.at[2], sems.at[3], peer
        ).start(),
    )
    far_in[pl.ds(me, 1)] = far_out[pl.ds(me, 1)]
    for copy in near:
        copy.wait_recv()
    near_total = near_count * near_rows
    table[0:near_total, :] = near_in[...].reshape(near_total, width)
    remote(far_out.at[others], far_in.at[others], sems.at[2], sems.at[3], me).wait_recv()
    pair = collect_rows(far_in, wide, peers, width)
    table[near_total : near_total + peers, :] = pair[0].astype(BF16)
    table[near_total + peers : near_total + 2 * peers, :] = pair[1].astype(BF16)
    for copy in near:
        copy.wait_send()
    remote(idx_out.at[others], idx_in.at[others], sems.at[0], sems.at[1], me).wait_send()
    remote(far_out.at[others], far_in.at[others], sems.at[2], sems.at[3], me).wait_send()


def return_kernel(
    peers, base, back, near_lists, coarse_slots,
    node_grad,
    near_out, near_in, wide, far_out, far_in, near_send, near_recv, sems,
):
    me = lax.axis_index("patch")
    own, width = base.shape
    near_count, near_rows = near_lists.shape
    near_total = near_count * near_rows
    barrier = greet_all(peers)
    near_out[...] = back[0:near_total, :].reshape(near_count, near_rows, width)
    pair = [
        back[near_total + s * peers : near_total + (s + 1) * peers, :].astype(F32)
        for s in range(2)
    ]
    spread_rows(pair, wide, far_out, peers)
    pl.semaphore_wait(barrier, peers - 1)
    offsets = offsets_of(near_count)
    near = []
    for k in range(near_count):
        copy = remote(
            near_out.at[k], near_in.at[k], near_send.at[k], near_recv.at[k],
            lax.rem(me - offsets[k] + peers, peers),
        )
        copy.start()
        near.append(copy)
    peers_loop(
        peers,
        lambda peer: remote(
            far_out.at[peer], far_in.at[me], sems.at[0], sems.at[1], peer
        ).start(),
    )
    far_in[pl.ds(me, 1)] = far_out[pl.ds(me, 1)]
    others = pl.ds(0, peers - 1)
    total = base[...]
    for k in range(near_count):
        near[k].wait_recv()
        mask = iota((own, near_rows), 0) == near_lists[k : k + 1, :]
        total = total + mm(hot(mask), near_in[k])
    slots = coarse_slots[...].T
    remote(far_out.at[others], far_in.at[others], sems.at[0], sems.at[1], me).wait_recv()
    pair = collect_rows(far_in, wide, peers, width)
    for s in range(2):
        mask = iota((own, peers), 0) == slots[s : s + 1, :]
        total = total + mm(hot(mask), pair[s].astype(BF16))
    node_grad[...] = total.astype(BF16)
    for copy in near:
        copy.wait_send()
    remote(far_out.at[others], far_in.at[others], sems.at[0], sems.at[1], me).wait_send()


def normal_stats(values):
    center = values - jnp.mean(values, axis=-1, keepdims=True)
    spread = jnp.mean(center * center, axis=-1, keepdims=True)
    inv = lax.rsqrt(spread + 1e-05)
    return center * inv, inv


def normal_back(grad, unit, inv):
    along = jnp.mean(grad * unit, axis=-1, keepdims=True)
    return inv * (grad - jnp.mean(grad, axis=-1, keepdims=True) - unit * along)


def silu_both(values):
    gate = 0.5 + 0.5 * jnp.tanh(0.5 * values)
    out = values * gate
    return out, gate + out * (1.0 - gate)


def compute_kernel(
    rows, peers, far_width,
    nodes, node_cot, table, send_rows, recv_rows, counts,
    edge_bias, edge_out_bias, edge_gain, node_bias, node_out_bias, node_gain,
    edges_h, edge_cot_h, w_edge_h, w_send_h, w_recv_h, w_edge_out_h, w_node_h, w_agg_h, w_node_out_h,
    new_nodes, base, back, new_edges_h, edge_grad_h,
    edges, edge_cot, w_edge, w_send, w_recv, w_edge_out, w_node, w_agg, w_node_out,
    new_edges, edge_grad, proj, onehot, onehot_t, slope, unit, invs, sent, dpre, dagg,
    in_sems, new_sems, grad_sems,
):
    own, width = nodes.shape
    total_edges = edges.shape[0]
    ext = table.shape[0]
    send_pad = -(-(ext + own) // LANES) * LANES
    recv_pad = -(-own // LANES) * LANES
    steps = total_edges // rows
    near_total = ext - far_width * peers

    moves = [
        (w_send_h, w_send), (w_recv_h, w_recv), (edges_h, edges), (w_edge_h, w_edge),
        (w_edge_out_h, w_edge_out), (w_agg_h, w_agg), (w_node_h, w_node),
        (w_node_out_h, w_node_out), (edge_cot_h, edge_cot),
    ]
    copies = [pltpu.make_async_copy(a, b, in_sems.at[i]) for i, (a, b) in enumerate(moves)]
    for copy in copies:
        copy.start()

    raw = send_rows[...]
    far = raw - own - near_total
    address = jnp.where(
        raw < own, raw + ext,
        jnp.where(raw < own + near_total, raw - own,
                  near_total + jnp.bitwise_and(far, 1) * peers + lax.shift_right_arithmetic(far, 1)),
    )
    target = recv_rows[...]

    groups = total_edges // LANES
    for g in range(groups):
        line = address[g : g + 1, :]
        goal = target[g : g + 1, :]
        span = slice(g * LANES, (g + 1) * LANES)
        onehot_t[0:send_pad, span] = hot(iota((send_pad, LANES), 0) == line)
        onehot_t[send_pad:, span] = hot(iota((recv_pad, LANES), 0) == goal)
        line_col = jnp.broadcast_to(line, (LANES, LANES)).T
        goal_col = jnp.broadcast_to(goal, (LANES, LANES)).T
        lane = iota((LANES, LANES), 1)
        for c in range(send_pad // LANES):
            onehot[span, c * LANES : (c + 1) * LANES] = hot(line_col == lane + c * LANES)
        for c in range(recv_pad // LANES):
            onehot[span, send_pad + c * LANES : send_pad + (c + 1) * LANES] = hot(
                goal_col == lane + c * LANES
            )

    proj[ext + own : send_pad, :] = jnp.zeros((send_pad - ext - own, width), BF16)
    proj[send_pad + own :, :] = jnp.zeros((recv_pad - own, width), BF16)
    dagg[own:, :] = jnp.zeros((recv_pad - own, width), BF16)
    copies[0].wait()
    proj[ext : ext + own, :] = mm(nodes[...], w_send[...]).astype(BF16)
    copies[1].wait()
    proj[send_pad : send_pad + own, :] = mm(nodes[...], w_recv[...]).astype(BF16)
    proj[0:ext, :] = mm(table[...], w_send[...]).astype(BF16)
    copies[2].wait()
    copies[3].wait()
    copies[4].wait()
    live_rows = counts[0] * BLOCK

    def forward(step, carry):
        at = pl.ds(pl.multiple_of(step * rows, rows), rows)
        pre = mm(edges[at, :], w_edge[...]) + mm(onehot[at, :], proj[...]) + edge_bias[...]
        hidden, rise = silu_both(pre)
        slope[at, :] = rise
        out = mm(hidden.astype(BF16), w_edge_out[...]) + edge_out_bias[...]
        normed, inv = normal_stats(out)
        unit[at, :] = normed
        invs[at, :] = jnp.broadcast_to(inv, (rows, LANES))
        alive = iota((rows, 1), 0) + step * rows < live_rows
        message = jnp.where(alive, edge_gain[...], 0.0) * normed
        sent[at, :] = message.astype(BF16)
        new_edges[at, :] = (edges[at, :].astype(F32) + message).astype(BF16)
        return carry

    lax.fori_loop(0, steps, forward, 0)
    new_copy = pltpu.make_async_copy(new_edges, new_edges_h, new_sems.at[0])

    aggregate = mm(onehot_t[send_pad : send_pad + own, :], sent[...]).astype(BF16)
    new_copy.start()
    for i in (5, 6, 7):
        copies[i].wait()
    pre = mm(nodes[...], w_node[...]) + mm(aggregate, w_agg[...]) + node_bias[...]
    hidden, rise = silu_both(pre)
    out = mm(hidden.astype(BF16), w_node_out[...]) + node_out_bias[...]
    normed, inv = normal_stats(out)
    new_nodes[...] = (nodes[...].astype(F32) + node_gain[...] * normed).astype(BF16)
    cot = node_cot[...].astype(F32)
    d_out = normal_back(node_gain[...] * cot, normed, inv).astype(BF16)
    d_pre = (mm_nt(d_out, w_node_out[...]) * rise).astype(BF16)
    dagg[0:own, :] = mm_nt(d_pre, w_agg[...]).astype(BF16)
    base[...] = cot + mm_nt(d_pre, w_node[...])
    copies[8].wait()

    def backward(step, carry):
        at = pl.ds(pl.multiple_of(step * rows, rows), rows)
        cot = edge_cot[at, :].astype(F32)
        d_message = cot + mm(onehot[at, send_pad:], dagg[...])
        alive = iota((rows, 1), 0) + step * rows < live_rows
        d_unit = jnp.where(alive, edge_gain[...], 0.0) * d_message
        d_out = normal_back(d_unit, unit[at, :], invs[at, 0:1]).astype(BF16)
        d_pre = (mm_nt(d_out, w_edge_out[...]) * slope[at, :]).astype(BF16)
        dpre[at, :] = d_pre
        edge_grad[at, :] = (cot + mm_nt(d_pre, w_edge[...])).astype(BF16)
        return carry

    lax.fori_loop(0, steps, backward, 0)
    grad_copy = pltpu.make_async_copy(edge_grad, edge_grad_h, grad_sems.at[0])

    sums = mm(onehot_t[0:ext, :], dpre[...]).astype(BF16)
    grad_copy.start()
    back[...] = mm_nt(sums, w_send[...]).astype(BF16)
    sums = mm(onehot_t[ext : ext + own, :], dpre[...]).astype(BF16)
    total = base[...] + mm_nt(sums, w_send[...])
    sums = mm(onehot_t[send_pad : send_pad + own, :], dpre[...]).astype(BF16)
    base[...] = total + mm_nt(sums, w_recv[...])
    new_copy.wait()
    grad_copy.wait()


VM = pl.BlockSpec(memory_space=pltpu.VMEM)
SM = pl.BlockSpec(memory_space=pltpu.SMEM)
ANY = pl.BlockSpec(memory_space=pl.ANY)
DMA = pltpu.SemaphoreType.DMA


def local(
    nodes, edges, node_cot, edge_cot, w_edge, w_send, w_recv, edge_bias, w_edge_out,
    edge_out_bias, edge_gain, w_node, w_agg, node_bias, w_node_out, node_out_bias, node_gain,
    send_slots, recv_slots, neighbour_send_lists, coarse_rows, far_lists, block_count,
):
    own, width = nodes.shape
    total_edges = edges.shape[0]
    peers = lax.axis_size("patch")
    near_count, near_rows = neighbour_send_lists.shape
    far_width = far_lists.shape[2]
    near_total = near_count * near_rows
    ext = near_total + far_width * peers
    unit_rows = far_width * width // LANES
    shape = jax.ShapeDtypeStruct
    exchange = [
        pltpu.VMEM((near_count, near_rows, width), BF16),
        pltpu.VMEM((near_count, near_rows, width), BF16),
    ]
    far_scratch = [
        pltpu.VMEM((peers * unit_rows, LANES), F32),
        pltpu.VMEM((peers, unit_rows, LANES), BF16),
        pltpu.VMEM((peers, unit_rows, LANES), BF16),
    ]
    table, coarse_slots = pl.pallas_call(
        functools.partial(send_kernel, peers),
        name="send_rows",
        out_shape=(shape((ext, width), BF16), shape((peers, LANES), jnp.int32)),
        in_specs=[VM, VM, VM, SM],
        out_specs=(VM, VM),
        scratch_shapes=exchange
        + [pltpu.VMEM((peers, 1, LANES), jnp.int32), pltpu.VMEM((peers, 1, LANES), jnp.int32)]
        + far_scratch
        + [DMA((near_count,)), DMA((near_count,)), DMA((4,))],
        compiler_params=pltpu.CompilerParams(collective_id=0, has_side_effects=True),
    )(nodes, neighbour_send_lists, far_lists, coarse_rows)

    rows = 256
    send_pad = -(-(ext + own) // LANES) * LANES
    recv_pad = -(-own // LANES) * LANES
    wide = lambda v: v.reshape(1, -1)
    weight = pltpu.VMEM((width, width), BF16)
    edge_b = pltpu.VMEM((total_edges, width), BF16)
    edge_f = pltpu.VMEM((total_edges, width), F32)
    new_nodes, base, back, new_edges, edge_grad = pl.pallas_call(
        functools.partial(compute_kernel, rows, peers, far_width),
        name="layer",
        out_shape=(
            shape((own, width), BF16), shape((own, width), F32), shape((ext, width), BF16),
            shape((total_edges, width), BF16), shape((total_edges, width), BF16),
        ),
        in_specs=[VM] * 5 + [SM] + [VM] * 6 + [ANY] * 9,
        out_specs=(VM, VM, VM, ANY, ANY),
        scratch_shapes=[edge_b, edge_b] + [weight] * 7
        + [
            edge_b, edge_b,
            pltpu.VMEM((send_pad + recv_pad, width), BF16),
            pltpu.VMEM((total_edges, send_pad + recv_pad), BF16),
            pltpu.VMEM((send_pad + recv_pad, total_edges), BF16),
            edge_f, edge_f,
            pltpu.VMEM((total_edges, LANES), F32),
            edge_b, edge_b,
            pltpu.VMEM((recv_pad, width), BF16),
            DMA((9,)), DMA((1,)), DMA((1,)),
        ],
        compiler_params=pltpu.CompilerParams(vmem_limit_bytes=56 << 20),
    )(
        nodes, node_cot, table, send_slots.reshape(-1, LANES), recv_slots.reshape(-1, LANES),
        block_count, wide(edge_bias), wide(edge_out_bias), wide(edge_gain), wide(node_bias),
        wide(node_out_bias), wide(node_gain),
        edges, edge_cot, w_edge, w_send, w_recv, w_edge_out, w_node, w_agg, w_node_out,
    )

    node_grad = pl.pallas_call(
        functools.partial(return_kernel, peers),
        name="return_rows",
        out_shape=shape((own, width), BF16),
        in_specs=[VM] * 4,
        out_specs=VM,
        scratch_shapes=exchange + far_scratch + [DMA((near_count,)), DMA((near_count,)), DMA((2,))],
        compiler_params=pltpu.CompilerParams(collective_id=1, has_side_effects=True),
    )(base, back, neighbour_send_lists, coarse_slots)
    return new_nodes, new_edges, node_grad, edge_grad


def solution(mesh):
    both = P(("groups", "patch"), None)
    placed = (both,) * 4 + (P(),) * 13 + (
        P("patch"), P("patch"), P("patch", None), P("patch"), P("patch", None, None), P("patch"),
    )
    return jax.shard_map(
        local, mesh=mesh, in_specs=placed, out_specs=(both,) * 4, check_vma=False
    )
```

```python
import functools

import jax
import jax.numpy as jnp
from jax import lax
from jax.experimental import pallas as pl
from jax.experimental.pallas import tpu as pltpu
from jax.sharding import PartitionSpec as P

BLOCK = 128
LANES = 128
MESH = pl.DeviceIdType.MESH
F32 = jnp.float32
BF16 = jnp.bfloat16
STRIDE = 75
VMEM_LIMIT = 60 << 20


def mm(a, b):
    return lax.dot_general(a, b, (((1,), (0,)), ((), ())), preferred_element_type=F32)


def mm_nt(a, b):
    return lax.dot_general(a, b, (((1,), (1,)), ((), ())), preferred_element_type=F32)


def mm_tn(a, b):
    return lax.dot_general(a, b, (((0,), (0,)), ((), ())), preferred_element_type=F32)


def iota(shape, dim):
    return lax.broadcasted_iota(jnp.int32, shape, dim)


def hot(mask):
    return jnp.where(mask, 1.0, 0.0).astype(BF16)


def offsets_of(count):
    return [(index // 2 + 1) * (1 - 2 * (index % 2)) for index in range(count)]


def peers_loop(peers, body):
    hop = STRIDE % peers

    def step(i, peer):
        peer = peer + hop
        peer = jnp.where(peer >= peers, peer - peers, peer)
        body(peer)
        return peer

    lax.fori_loop(1, peers, step, lax.axis_index("patch"))


def greet_all(peers):
    barrier = pltpu.get_barrier_semaphore()

    def greet(peer):
        pl.semaphore_signal(barrier, inc=1, device_id={"patch": peer}, device_id_type=MESH)

    peers_loop(peers, greet)
    return barrier


def remote(src, dst, send, recv, peer):
    return pltpu.make_async_remote_copy(
        src_ref=src, dst_ref=dst, send_sem=send, recv_sem=recv,
        device_id={"patch": peer}, device_id_type=MESH,
    )


def spread_rows(pair, wide, packed, peers):
    parts = pair[0].shape[1] // LANES
    unit = 2 * parts
    for slot in range(2):
        for part in range(parts):
            wide[pl.ds(2 * part + slot, peers, stride=unit), :] = pair[slot][
                :, part * LANES : (part + 1) * LANES
            ]
    packed[...] = wide[...].reshape(peers, unit, LANES).astype(BF16)


def collect_rows(packed, wide, peers, width):
    parts = width // LANES
    unit = 2 * parts
    wide[...] = packed[...].astype(F32).reshape(peers * unit, LANES)
    pair = []
    for slot in range(2):
        pieces = [
            wide[pl.ds(2 * part + slot, peers, stride=unit), :] for part in range(parts)
        ]
        pair.append(jnp.concatenate(pieces, axis=1))
    return pair


def normal_stats(values):
    center = values - jnp.mean(values, axis=-1, keepdims=True)
    spread = jnp.mean(center * center, axis=-1, keepdims=True)
    inv = lax.rsqrt(spread + 1e-05)
    return center * inv, inv


def normal_back(grad, unit, inv):
    along = jnp.mean(grad * unit, axis=-1, keepdims=True)
    return inv * (grad - jnp.mean(grad, axis=-1, keepdims=True) - unit * along)


def silu_both(values):
    gate = 0.5 + 0.5 * jnp.tanh(0.5 * values)
    out = values * gate
    return out, gate + out * (1.0 - gate)


def layer_kernel(
    rows, peers,
    coarse, counts,
    nodes_h, near_lists_h, far_lists_h, send_rows_h, recv_rows_h, node_cot_h,
    edge_bias_h, edge_out_bias_h, edge_gain_h, node_bias_h, node_out_bias_h, node_gain_h,
    edges_h, edge_cot_h, w_edge_h, w_send_h, w_recv_h, w_edge_out_h, w_node_h, w_agg_h, w_node_out_h,
    new_nodes, new_edges, node_grad, edge_grad,
    near_out, near_in, near_out_b, near_in_b, idx_out, idx_in, wide,
    far_out, far_in, far_out_b, far_in_b,
    nodes, near_lists, far_lists, send_rows, recv_rows, node_cot,
    edge_bias, edge_out_bias, edge_gain, node_bias, node_out_bias, node_gain,
    edges, edge_cot, w_edge, w_send, w_recv, w_edge_out, w_node, w_agg, w_node_out,
    proj, onehot, onehot_t, slope, unit, invs, sent, dpre, dagg,
    near_send, near_recv, near_send_b, near_recv_b, sems, in_sems,
):
    me = lax.axis_index("patch")
    own, width = nodes.shape
    total_edges = edges.shape[0]
    near_count, near_rows = near_lists.shape
    near_total = near_count * near_rows
    ext = near_total + 2 * peers
    send_pad = -(-(ext + own) // LANES) * LANES
    recv_pad = -(-own // LANES) * LANES
    steps = total_edges // rows
    offsets = offsets_of(near_count)
    others = pl.ds(0, peers - 1)

    barrier = greet_all(peers)
    moves = [
        (nodes_h, nodes), (near_lists_h, near_lists), (far_lists_h, far_lists),
        (send_rows_h, send_rows), (recv_rows_h, recv_rows), (edge_bias_h, edge_bias),
        (edge_out_bias_h, edge_out_bias), (edge_gain_h, edge_gain), (node_bias_h, node_bias),
        (node_out_bias_h, node_out_bias), (node_gain_h, node_gain), (node_cot_h, node_cot),
        (w_send_h, w_send), (w_recv_h, w_recv), (edges_h, edges), (w_edge_h, w_edge),
        (w_edge_out_h, w_edge_out), (w_agg_h, w_agg), (w_node_h, w_node),
        (w_node_out_h, w_node_out), (edge_cot_h, edge_cot),
    ]
    copies = [pltpu.make_async_copy(a, b, in_sems.at[i]) for i, (a, b) in enumerate(moves)]
    for copy in copies:
        copy.start()
    first_big = len(copies) - 9

    for i in range(3):
        copies[i].wait()
    for k in range(near_count):
        mask = iota((own, near_rows), 0) == near_lists[k : k + 1, :]
        near_out[k] = mm_tn(hot(mask), nodes[...]).astype(BF16)
    first = jnp.broadcast_to(far_lists[0, 0:1, :], (LANES, peers))
    second = jnp.broadcast_to(far_lists[0, 1:2, :], (LANES, peers))
    wanted = jnp.where(iota((LANES, peers), 0) == 0, first, second).T
    idx_out[...] = wanted.reshape(peers, 1, LANES)

    pl.semaphore_wait(barrier, peers - 1)
    peers_loop(
        peers,
        lambda peer: remote(
            idx_out.at[peer], idx_in.at[me], sems.at[0], sems.at[1], peer
        ).start(),
    )
    near = []
    for k in range(near_count):
        copy = remote(
            near_out.at[k], near_in.at[k], near_send.at[k], near_recv.at[k],
            lax.rem(me + offsets[k] + peers, peers),
        )
        copy.start()
        near.append(copy)
    idx_in[pl.ds(me, 1)] = idx_out[pl.ds(me, 1)]

    for i in range(3, first_big):
        copies[i].wait()
    copies = copies[first_big:]
    raw = send_rows[...]
    far = raw - own - near_total
    address = jnp.where(
        raw < own, raw + ext,
        jnp.where(raw < own + near_total, raw - own,
                  near_total + jnp.bitwise_and(far, 1) * peers + lax.shift_right_arithmetic(far, 1)),
    )
    target = recv_rows[...]
    lane = iota((LANES, LANES), 1)
    for g in range(total_edges // LANES):
        line = address[g : g + 1, :]
        goal = target[g : g + 1, :]
        span = slice(g * LANES, (g + 1) * LANES)
        onehot_t[0:send_pad, span] = hot(iota((send_pad, LANES), 0) == line)
        onehot_t[send_pad:, span] = hot(iota((recv_pad, LANES), 0) == goal)
        line_col = jnp.broadcast_to(line, (LANES, LANES)).T
        goal_col = jnp.broadcast_to(goal, (LANES, LANES)).T
        for c in range(send_pad // LANES):
            onehot[span, c * LANES : (c + 1) * LANES] = hot(line_col == lane + c * LANES)
        for c in range(recv_pad // LANES):
            onehot[span, send_pad + c * LANES : send_pad + (c + 1) * LANES] = hot(
                goal_col == lane + c * LANES
            )
    proj[ext + own : send_pad, :] = jnp.zeros((send_pad - ext - own, width), BF16)
    proj[send_pad + own :, :] = jnp.zeros((recv_pad - own, width), BF16)
    dagg[own:, :] = jnp.zeros((recv_pad - own, width), BF16)
    copies[0].wait()
    proj[ext : ext + own, :] = mm(nodes[...], w_send[...]).astype(BF16)
    copies[1].wait()
    proj[send_pad : send_pad + own, :] = mm(nodes[...], w_recv[...]).astype(BF16)
    copies[2].wait()
    copies[3].wait()
    for copy in near:
        copy.wait_recv()
    proj[0:near_total, :] = mm(near_in[...].reshape(near_total, width), w_send[...]).astype(BF16)

    def ahead(step, carry):
        at = pl.ds(pl.multiple_of(step * rows, rows), rows)
        slope[at, :] = (
            mm(edges[at, :], w_edge[...])
            + mm(onehot[at, 0:near_total], proj[0:near_total, :])
            + mm(onehot[at, ext:], proj[ext:, :])
            + edge_bias[...]
        )
        return carry

    lax.fori_loop(0, steps, ahead, 0)

    remote(idx_out.at[others], idx_in.at[others], sems.at[0], sems.at[1], me).wait_recv()
    asked = idx_in[...].reshape(peers, LANES)
    slots = jnp.zeros_like(asked)
    for c in range(coarse.shape[0]):
        slots = jnp.where(asked == c, coarse[c], slots)
    pair = [mm(hot(iota((peers, own), 1) == slots[:, s : s + 1]), nodes[...]) for s in range(2)]
    spread_rows(pair, wide, far_out, peers)
    peers_loop(
        peers,
        lambda peer: remote(
            far_out.at[peer], far_in.at[me], sems.at[2], sems.at[3], peer
        ).start(),
    )
    far_in[pl.ds(me, 1)] = far_out[pl.ds(me, 1)]
    slots_t = slots.T
    for i in (4, 5, 6, 7, 8):
        copies[i].wait()
    node_pre = mm(nodes[...], w_node[...]) + node_bias[...]
    live_rows = counts[0] * BLOCK

    remote(far_out.at[others], far_in.at[others], sems.at[2], sems.at[3], me).wait_recv()
    pair = collect_rows(far_in, wide, peers, width)
    for s in range(2):
        proj[near_total + s * peers : near_total + (s + 1) * peers, :] = mm(
            pair[s].astype(BF16), w_send[...]
        ).astype(BF16)

    def forward(step, carry):
        at = pl.ds(pl.multiple_of(step * rows, rows), rows)
        pre = slope[at, :] + mm(onehot[at, near_total:ext], proj[near_total:ext, :])
        hidden, rise = silu_both(pre)
        slope[at, :] = rise
        out = mm(hidden.astype(BF16), w_edge_out[...]) + edge_out_bias[...]
        normed, inv = normal_stats(out)
        unit[at, :] = normed
        invs[at, :] = jnp.broadcast_to(inv, (rows, LANES))
        alive = iota((rows, 1), 0) + step * rows < live_rows
        message = jnp.where(alive, edge_gain[...], 0.0) * normed
        sent[at, :] = message.astype(BF16)
        new_edges[at, :] = (edges[at, :].astype(F32) + message).astype(BF16)
        return carry

    lax.fori_loop(0, steps, forward, 0)

    aggregate = mm(onehot_t[send_pad : send_pad + own, :], sent[...]).astype(BF16)
    pre = node_pre + mm(aggregate, w_agg[...])
    hidden, rise = silu_both(pre)
    out = mm(hidden.astype(BF16), w_node_out[...]) + node_out_bias[...]
    normed, inv = normal_stats(out)
    new_nodes[...] = (nodes[...].astype(F32) + node_gain[...] * normed).astype(BF16)
    node_back = node_cot[...].astype(F32)
    d_out = normal_back(node_gain[...] * node_back, normed, inv).astype(BF16)
    d_node = (mm_nt(d_out, w_node_out[...]) * rise).astype(BF16)
    dagg[0:own, :] = mm_nt(d_node, w_agg[...]).astype(BF16)

    def backward(step, carry):
        at = pl.ds(pl.multiple_of(step * rows, rows), rows)
        d_message = edge_cot[at, :].astype(F32) + mm(onehot[at, send_pad:], dagg[...])
        alive = iota((rows, 1), 0) + step * rows < live_rows
        d_unit = jnp.where(alive, edge_gain[...], 0.0) * d_message
        d_out = normal_back(d_unit, unit[at, :], invs[at, 0:1]).astype(BF16)
        dpre[at, :] = (mm_nt(d_out, w_edge_out[...]) * slope[at, :]).astype(BF16)
        return carry

    lax.fori_loop(0, steps, backward, 0)

    sums = mm(onehot_t[0:ext, :], dpre[...]).astype(BF16)
    back = mm_nt(sums, w_send[...])
    near_out_b[...] = back[0:near_total, :].astype(BF16).reshape(near_count, near_rows, width)
    pair = [back[near_total + s * peers : near_total + (s + 1) * peers, :] for s in range(2)]
    spread_rows(pair, wide, far_out_b, peers)
    peers_loop(
        peers,
        lambda peer: remote(
            far_out_b.at[peer], far_in_b.at[me], sems.at[4], sems.at[5], peer
        ).start(),
    )
    near_b = []
    for k in range(near_count):
        copy = remote(
            near_out_b.at[k], near_in_b.at[k], near_send_b.at[k], near_recv_b.at[k],
            lax.rem(me - offsets[k] + peers, peers),
        )
        copy.start()
        near_b.append(copy)
    far_in_b[pl.ds(me, 1)] = far_out_b[pl.ds(me, 1)]

    sums = mm(onehot_t[ext : ext + own, :], dpre[...]).astype(BF16)
    total = node_back + mm_nt(d_node, w_node[...]) + mm_nt(sums, w_send[...])
    sums = mm(onehot_t[send_pad : send_pad + own, :], dpre[...]).astype(BF16)
    total = total + mm_nt(sums, w_recv[...])

    def finish(step, carry):
        at = pl.ds(pl.multiple_of(step * rows, rows), rows)
        grad = edge_cot[at, :].astype(F32) + mm_nt(dpre[at, :], w_edge[...])
        edge_grad[at, :] = grad.astype(BF16)
        return carry

    lax.fori_loop(0, steps, finish, 0)

    for k in range(near_count):
        near_b[k].wait_recv()
        mask = iota((own, near_rows), 0) == near_lists[k : k + 1, :]
        total = total + mm(hot(mask), near_in_b[k])
    remote(far_out_b.at[others], far_in_b.at[others], sems.at[4], sems.at[5], me).wait_recv()
    pair = collect_rows(far_in_b, wide, peers, width)
    for s in range(2):
        mask = iota((own, peers), 0) == slots_t[s : s + 1, :]
        total = total + mm(hot(mask), pair[s].astype(BF16))
    node_grad[...] = total.astype(BF16)
    for copy in near:
        copy.wait_send()
    for copy in near_b:
        copy.wait_send()
    remote(idx_out.at[others], idx_in.at[others], sems.at[0], sems.at[1], me).wait_send()
    remote(far_out.at[others], far_in.at[others], sems.at[2], sems.at[3], me).wait_send()
    remote(far_out_b.at[others], far_in_b.at[others], sems.at[4], sems.at[5], me).wait_send()


def place_kernel(a, b, c, d, a_out, b_out, c_out, d_out, sems):
    pairs = ((b, b_out), (d, d_out), (a, a_out), (c, c_out))
    copies = [pltpu.make_async_copy(x, y, sems.at[i]) for i, (x, y) in enumerate(pairs)]
    for copy in copies:
        copy.start()
    for copy in copies:
        copy.wait()


VM = pl.BlockSpec(memory_space=pltpu.VMEM)
SM = pl.BlockSpec(memory_space=pltpu.SMEM)
HBM = pl.BlockSpec(memory_space=pltpu.HBM)
ANY = pl.BlockSpec(memory_space=pl.ANY)
DMA = pltpu.SemaphoreType.DMA
ROWS = 512


def local(
    nodes, edges, node_cot, edge_cot, w_edge, w_send, w_recv, edge_bias, w_edge_out,
    edge_out_bias, edge_gain, w_node, w_agg, node_bias, w_node_out, node_out_bias, node_gain,
    send_slots, recv_slots, neighbour_send_lists, coarse_rows, far_lists, block_count,
):
    own, width = nodes.shape
    total_edges = edges.shape[0]
    peers = lax.axis_size("patch")
    near_count, near_rows = neighbour_send_lists.shape
    near_total = near_count * near_rows
    ext = near_total + 2 * peers
    unit_rows = 2 * width // LANES
    send_pad = -(-(ext + own) // LANES) * LANES
    recv_pad = -(-own // LANES) * LANES
    flat = lambda v: v.reshape(1, -1)
    near_b = pltpu.VMEM((near_count, near_rows, width), BF16)
    index_b = pltpu.VMEM((peers, 1, LANES), jnp.int32)
    far_b = pltpu.VMEM((peers, unit_rows, LANES), BF16)
    node_b = pltpu.VMEM((own, width), BF16)
    slot_b = pltpu.VMEM((total_edges // LANES, LANES), jnp.int32)
    weight = pltpu.VMEM((width, width), BF16)
    edge_b = pltpu.VMEM((total_edges, width), BF16)
    edge_f = pltpu.VMEM((total_edges, width), F32)
    shapes = tuple(
        jax.ShapeDtypeStruct((n, width), BF16) for n in (own, total_edges, own, total_edges)
    )
    results = pl.pallas_call(
        functools.partial(layer_kernel, ROWS, peers),
        name="layer",
        out_shape=tuple(pltpu.VMEM(v.shape, v.dtype) for v in shapes),
        in_specs=[SM] * 2 + [HBM] * 21,
        out_specs=(VM,) * 4,
        scratch_shapes=[near_b] * 4 + [index_b] * 2
        + [pltpu.VMEM((peers * unit_rows, LANES), F32)] + [far_b] * 4
        + [
            node_b, pltpu.VMEM(neighbour_send_lists.shape, jnp.int32), pltpu.VMEM((1, 2, peers), jnp.int32),
            slot_b, slot_b, node_b,
        ]
        + [pltpu.VMEM((1, width), F32)] * 6
        + [edge_b] * 2 + [weight] * 7
        + [
            pltpu.VMEM((send_pad + recv_pad, width), BF16),
            pltpu.VMEM((total_edges, send_pad + recv_pad), BF16),
            pltpu.VMEM((send_pad + recv_pad, total_edges), BF16),
            edge_f, edge_f,
            pltpu.VMEM((total_edges, LANES), F32),
            edge_b, edge_b,
            pltpu.VMEM((recv_pad, width), BF16),
        ]
        + [DMA((near_count,))] * 4 + [DMA((6,)), DMA((21,))],
        compiler_params=pltpu.CompilerParams(
            collective_id=0, has_side_effects=True, vmem_limit_bytes=VMEM_LIMIT
        ),
    )(
        coarse_rows, block_count, nodes, neighbour_send_lists, far_lists.transpose(0, 2, 1),
        send_slots.reshape(-1, LANES), recv_slots.reshape(-1, LANES), node_cot,
        flat(edge_bias), flat(edge_out_bias), flat(edge_gain), flat(node_bias),
        flat(node_out_bias), flat(node_gain),
        edges, edge_cot, w_edge, w_send, w_recv, w_edge_out, w_node, w_agg, w_node_out,
    )
    return pl.pallas_call(
        place_kernel,
        name="place",
        out_shape=shapes,
        in_specs=[VM] * 4,
        out_specs=(ANY,) * 4,
        scratch_shapes=[DMA((4,))],
        compiler_params=pltpu.CompilerParams(vmem_limit_bytes=8 << 20),
    )(*results)


def solution(mesh):
    both = P(("groups", "patch"), None)
    placed = (both,) * 4 + (P(),) * 13 + (
        P("patch"), P("patch"), P("patch", None), P("patch"), P("patch", None, None), P("patch"),
    )
    return jax.shard_map(
        local, mesh=mesh, in_specs=placed, out_specs=(both,) * 4, check_vma=False
    )
```

```python
import functools
import math

import jax
import jax.numpy as jnp
from jax import lax
from jax.experimental import pallas as pl
from jax.experimental.pallas import tpu as pltpu
from jax.sharding import PartitionSpec as P

BLOCK = 128
LANES = 128
MESH = pl.DeviceIdType.MESH
F32 = jnp.float32
BF16 = jnp.bfloat16
VMEM_LIMIT = 60 << 20


def mm(a, b):
    return lax.dot_general(a, b, (((1,), (0,)), ((), ())), preferred_element_type=F32)


def mm_nt(a, b):
    return lax.dot_general(a, b, (((1,), (1,)), ((), ())), preferred_element_type=F32)


def mm_tn(a, b):
    return lax.dot_general(a, b, (((0,), (0,)), ((), ())), preferred_element_type=F32)


def iota(shape, dim):
    return lax.broadcasted_iota(jnp.int32, shape, dim)


def hot(mask):
    return jnp.where(mask, 1.0, 0.0).astype(BF16)


def offsets_of(count):
    return [(index // 2 + 1) * (1 - 2 * (index % 2)) for index in range(count)]


def side_of(peers):
    return math.isqrt(peers // 2)


def far_first(side):
    half = side // 2
    return sorted(range(1, side), key=lambda k: -min(k, side - k)) if half else []


def place_of(me, side):
    core = lax.rem(me, 2)
    line = lax.rem(lax.div(me, 2), side)
    return lax.div(me, 2 * side), line, core


def wrapped(value, side):
    return jnp.where(value >= side, value - side, value)


def every_peer(me, side, body):
    x, y, core = place_of(me, side)
    within = [(oy, oc) for oy in far_first(side) + [0] for oc in (0, 1)]
    lines = {oy: 2 * wrapped(y + oy, side) for oy in range(side)}
    cores = (core, 1 - core)

    def step(i, carry):
        away = lax.div(i + 1, 2) * (1 - 2 * lax.rem(i, 2))
        row = wrapped(x + side // 2 + away, side) * (2 * side)
        for oy, oc in within:
            body(row + lines[oy] + cores[oc])
        return carry

    lax.fori_loop(0, side - 1, step, 0)
    for oy, oc in within[:-2] + [(0, 1)]:
        body(x * (2 * side) + lines[oy] + cores[oc])


def remote(src, dst, send, recv, peer):
    return pltpu.make_async_remote_copy(
        src_ref=src, dst_ref=dst, send_sem=send, recv_sem=recv,
        device_id={"patch": peer}, device_id_type=MESH,
    )


def spread_rows(pair, wide, packed, peers):
    parts = pair[0].shape[1] // LANES
    unit = 2 * parts
    for slot in range(2):
        for part in range(parts):
            wide[pl.ds(2 * part + slot, peers, stride=unit), :] = pair[slot][
                :, part * LANES : (part + 1) * LANES
            ]
    packed[...] = wide[...].reshape(peers, unit, LANES).astype(BF16)


def collect_rows(packed, wide, peers, width):
    parts = width // LANES
    unit = 2 * parts
    wide[...] = packed[...].astype(F32).reshape(peers * unit, LANES)
    pair = []
    for slot in range(2):
        pieces = [
            wide[pl.ds(2 * part + slot, peers, stride=unit), :] for part in range(parts)
        ]
        pair.append(jnp.concatenate(pieces, axis=1))
    return pair


def normal_stats(values):
    center = values - jnp.mean(values, axis=-1, keepdims=True)
    spread = jnp.mean(center * center, axis=-1, keepdims=True)
    inv = lax.rsqrt(spread + 1e-05)
    return center * inv, inv


def normal_back(grad, unit, inv):
    along = jnp.mean(grad * unit, axis=-1, keepdims=True)
    return inv * (grad - jnp.mean(grad, axis=-1, keepdims=True) - unit * along)


def silu_both(values):
    gate = 0.5 + 0.5 * jnp.tanh(0.5 * values)
    out = values * gate
    return out, gate + out * (1.0 - gate)


def layer_kernel(
    rows, peers,
    coarse, counts,
    nodes_h, near_lists_h, far_lists_h, send_rows_h, recv_rows_h, node_cot_h,
    edge_bias_h, edge_out_bias_h, edge_gain_h, node_bias_h, node_out_bias_h, node_gain_h,
    edges_h, edge_cot_h, w_edge_h, w_send_h, w_recv_h, w_edge_out_h, w_node_h, w_agg_h, w_node_out_h,
    new_nodes, new_edges, node_grad, edge_grad,
    near_out, near_in, near_out_b, near_in_b, wide, far_out_b, far_in_b,
    row1, row2, row3, idx1, idx2, idx3, picks,
    nodes, near_lists, far_lists, send_rows, recv_rows, node_cot,
    edge_bias, edge_out_bias, edge_gain, node_bias, node_out_bias, node_gain,
    edges, edge_cot, w_edge, w_send, w_recv, w_edge_out, w_node, w_agg, w_node_out,
    proj, onehot, onehot_t, slope, unit, invs, sent, dpre, dagg,
    near_send, near_recv, near_send_b, near_recv_b, sems, hop_sems, in_sems,
):
    me = lax.axis_index("patch")
    own, width = nodes.shape
    total_edges = edges.shape[0]
    near_count, near_rows = near_lists.shape
    near_total = near_count * near_rows
    ext = near_total + 2 * peers
    send_pad = -(-(ext + own) // LANES) * LANES
    recv_pad = -(-own // LANES) * LANES
    steps = total_edges // rows
    offsets = offsets_of(near_count)
    others = pl.ds(0, peers - 1)

    side = side_of(peers)
    x, y, core = place_of(me, side)
    first_step = jnp.where(core == 0, 2 * side, 2)
    second_step = jnp.where(core == 0, 2, 2 * side)
    first_at = jnp.where(core == 0, x, y)
    second_at = jnp.where(core == 0, y, x)
    partner = me + 1 - 2 * core
    order = far_first(side)
    first_peers = [me + (wrapped(first_at + k, side) - first_at) * first_step for k in order]
    second_peers = [me + (wrapped(second_at + k, side) - second_at) * second_step for k in order]
    near_peers = [lax.rem(me + o + peers, peers) for o in offsets]
    barrier = pltpu.get_barrier_semaphore()
    known = first_peers + second_peers + near_peers + [partner]
    for peer in known:
        pl.semaphore_signal(barrier, inc=1, device_id={"patch": peer}, device_id_type=MESH)
    moves = [
        (nodes_h, nodes), (near_lists_h, near_lists), (far_lists_h, far_lists),
        (send_rows_h, send_rows), (recv_rows_h, recv_rows), (edge_bias_h, edge_bias),
        (edge_out_bias_h, edge_out_bias), (edge_gain_h, edge_gain), (node_bias_h, node_bias),
        (node_out_bias_h, node_out_bias), (node_gain_h, node_gain), (node_cot_h, node_cot),
        (w_send_h, w_send), (w_recv_h, w_recv), (edges_h, edges), (w_edge_h, w_edge),
        (w_edge_out_h, w_edge_out), (w_agg_h, w_agg), (w_node_h, w_node),
        (w_node_out_h, w_node_out), (edge_cot_h, edge_cot),
    ]
    copies = [pltpu.make_async_copy(a, b, in_sems.at[i]) for i, (a, b) in enumerate(moves)]
    for copy in copies:
        copy.start()
    first_big = len(copies) - 9

    for i in range(3):
        copies[i].wait()
    coarse_count = coarse.shape[0]
    chosen = jnp.zeros((coarse_count, own), jnp.int32)
    for c in range(coarse_count):
        chosen = jnp.where(iota(chosen.shape, 0) == c, coarse[c], chosen)
    rows_out = mm(hot(iota(chosen.shape, 1) == chosen), nodes[...]).astype(BF16)
    row1[pl.ds(first_at, 1)] = rows_out.reshape(1, coarse_count, width)
    idx1[pl.ds(first_at, 1)] = far_lists[...]

    pl.semaphore_wait(barrier, len(known))
    mine = row1.at[first_at]
    for peer in first_peers:
        remote(mine, mine, sems.at[0], sems.at[1], peer).start()
    for k in range(near_count):
        mask = iota((own, near_rows), 0) == near_lists[k : k + 1, :]
        near_out[k] = mm_tn(hot(mask), nodes[...]).astype(BF16)
    near = []
    for k in range(near_count):
        copy = remote(near_out.at[k], near_in.at[k], near_send.at[k], near_recv.at[k], near_peers[k])
        copy.start()
        near.append(copy)
    mine = idx1.at[first_at]
    for peer in first_peers:
        remote(mine, mine, sems.at[2], sems.at[3], peer).start()

    for i in range(3, first_big):
        copies[i].wait()
    copies = copies[first_big:]
    raw = send_rows[...]
    far = raw - own - near_total
    address = jnp.where(
        raw < own, raw + ext,
        jnp.where(raw < own + near_total, raw - own,
                  near_total + jnp.bitwise_and(far, 1) * peers + lax.shift_right_arithmetic(far, 1)),
    )
    target = recv_rows[...]
    lane = iota((LANES, LANES), 1)
    for g in range(total_edges // LANES):
        line = address[g : g + 1, :]
        goal = target[g : g + 1, :]
        span = slice(g * LANES, (g + 1) * LANES)
        onehot_t[0:send_pad, span] = hot(iota((send_pad, LANES), 0) == line)
        onehot_t[send_pad:, span] = hot(iota((recv_pad, LANES), 0) == goal)
        line_col = jnp.broadcast_to(line, (LANES, LANES)).T
        goal_col = jnp.broadcast_to(goal, (LANES, LANES)).T
        for c in range(send_pad // LANES):
            onehot[span, c * LANES : (c + 1) * LANES] = hot(line_col == lane + c * LANES)
        for c in range(recv_pad // LANES):
            onehot[span, send_pad + c * LANES : send_pad + (c + 1) * LANES] = hot(
                goal_col == lane + c * LANES
            )
    area = side * side
    q = iota((1, peers), 1)
    q_core = jnp.bitwise_and(q, 1)
    q_chip = lax.shift_right_logical(q, 1)
    q_x = q_chip // side
    q_y = q_chip - q_x * side
    key = jnp.where(q_core == 0, q_y * side + q_x, q_x * side + q_y)
    key = key + jnp.where(q_core == core, 0, area)
    for slot in range(2):
        spot = key * coarse_count + far_lists[0, slot : slot + 1, :]
        spot_col = jnp.broadcast_to(spot, (LANES, peers)).T
        picks[slot * peers : (slot + 1) * peers, :] = hot(
            iota((peers, 2 * area * coarse_count), 1) == spot_col[:, 0:1]
        )

    fewer = pl.ds(0, side - 1)
    remote(row1.at[fewer], row1.at[fewer], sems.at[0], sems.at[1], partner).wait_recv()
    hops = []
    for i, peer in enumerate(second_peers):
        copy = remote(row1, row2.at[second_at], hop_sems.at[0, i], hop_sems.at[1, i], peer)
        copy.start()
        hops.append(copy)
    remote(row1, row3.at[second_at], sems.at[4], sems.at[5], partner).start()
    row2[pl.ds(second_at, 1)] = row1[...].reshape(1, side, coarse_count, width)
    remote(idx1.at[fewer], idx1.at[fewer], sems.at[2], sems.at[3], partner).wait_recv()
    for peer in second_peers:
        remote(idx1, idx2.at[second_at], sems.at[6], sems.at[7], peer).start()
    idx2[pl.ds(second_at, 1)] = idx1[...].reshape(1, side, 2, peers)

    proj[ext + own : send_pad, :] = jnp.zeros((send_pad - ext - own, width), BF16)
    proj[send_pad + own :, :] = jnp.zeros((recv_pad - own, width), BF16)
    dagg[own:, :] = jnp.zeros((recv_pad - own, width), BF16)
    copies[0].wait()
    proj[ext : ext + own, :] = mm(nodes[...], w_send[...]).astype(BF16)
    copies[1].wait()
    proj[send_pad : send_pad + own, :] = mm(nodes[...], w_recv[...]).astype(BF16)
    copies[2].wait()
    copies[3].wait()
    for copy in near:
        copy.wait_recv()
    proj[0:near_total, :] = mm(near_in[...].reshape(near_total, width), w_send[...]).astype(BF16)

    def ahead(step, carry):
        at = pl.ds(pl.multiple_of(step * rows, rows), rows)
        slope[at, :] = (
            mm(edges[at, :], w_edge[...])
            + mm(onehot[at, 0:near_total], proj[0:near_total, :])
            + mm(onehot[at, ext:], proj[ext:, :])
            + edge_bias[...]
        )
        return carry

    lax.fori_loop(0, steps, ahead, 0)

    for i in reversed(range(len(order))):
        hops[i].wait_recv()
        origin = wrapped(second_at + side - order[i], side)
        remote(row2.at[origin], row3.at[origin], sems.at[4], sems.at[5], partner).start()
    remote(idx2.at[fewer], idx2.at[fewer], sems.at[6], sems.at[7], partner).wait_recv()
    remote(idx2, idx3, sems.at[8], sems.at[9], partner).start()
    for i in (4, 5, 6, 7, 8):
        copies[i].wait()
    node_pre = mm(nodes[...], w_node[...]) + node_bias[...]
    live_rows = counts[0] * BLOCK

    half = area * coarse_count
    mine_rows = mm(picks[:, 0:half], row2[...].reshape(half, width))
    remote(row2, row3, sems.at[4], sems.at[5], partner).wait_recv()
    far_rows = mine_rows + mm(picks[:, half:], row3[...].reshape(half, width))
    proj[near_total:ext, :] = mm(far_rows.astype(BF16), w_send[...]).astype(BF16)

    def forward(step, carry):
        at = pl.ds(pl.multiple_of(step * rows, rows), rows)
        pre = slope[at, :] + mm(onehot[at, near_total:ext], proj[near_total:ext, :])
        hidden, rise = silu_both(pre)
        slope[at, :] = rise
        out = mm(hidden.astype(BF16), w_edge_out[...]) + edge_out_bias[...]
        normed, inv = normal_stats(out)
        unit[at, :] = normed
        invs[at, :] = jnp.broadcast_to(inv, (rows, LANES))
        alive = iota((rows, 1), 0) + step * rows < live_rows
        message = jnp.where(alive, edge_gain[...], 0.0) * normed
        sent[at, :] = message.astype(BF16)
        new_edges[at, :] = (edges[at, :].astype(F32) + message).astype(BF16)
        return carry

    lax.fori_loop(0, steps, forward, 0)

    aggregate = mm(onehot_t[send_pad : send_pad + own, :], sent[...]).astype(BF16)
    pre = node_pre + mm(aggregate, w_agg[...])
    hidden, rise = silu_both(pre)
    out = mm(hidden.astype(BF16), w_node_out[...]) + node_out_bias[...]
    normed, inv = normal_stats(out)
    new_nodes[...] = (nodes[...].astype(F32) + node_gain[...] * normed).astype(BF16)
    node_back = node_cot[...].astype(F32)
    d_out = normal_back(node_gain[...] * node_back, normed, inv).astype(BF16)
    d_node = (mm_nt(d_out, w_node_out[...]) * rise).astype(BF16)
    dagg[0:own, :] = mm_nt(d_node, w_agg[...]).astype(BF16)

    def backward(step, carry):
        at = pl.ds(pl.multiple_of(step * rows, rows), rows)
        d_message = edge_cot[at, :].astype(F32) + mm(onehot[at, send_pad:], dagg[...])
        alive = iota((rows, 1), 0) + step * rows < live_rows
        d_unit = jnp.where(alive, edge_gain[...], 0.0) * d_message
        d_out = normal_back(d_unit, unit[at, :], invs[at, 0:1]).astype(BF16)
        dpre[at, :] = (mm_nt(d_out, w_edge_out[...]) * slope[at, :]).astype(BF16)
        return carry

    lax.fori_loop(0, steps, backward, 0)

    sums = mm(onehot_t[0:ext, :], dpre[...]).astype(BF16)
    back = mm_nt(sums, w_send[...])
    near_out_b[...] = back[0:near_total, :].astype(BF16).reshape(near_count, near_rows, width)
    pair = [back[near_total + s * peers : near_total + (s + 1) * peers, :] for s in range(2)]
    spread_rows(pair, wide, far_out_b, peers)
    every_peer(
        me, side,
        lambda peer: remote(
            far_out_b.at[peer], far_in_b.at[me], sems.at[10], sems.at[11], peer
        ).start(),
    )
    near_b = []
    for k in range(near_count):
        copy = remote(
            near_out_b.at[k], near_in_b.at[k], near_send_b.at[k], near_recv_b.at[k],
            lax.rem(me - offsets[k] + peers, peers),
        )
        copy.start()
        near_b.append(copy)
    far_in_b[pl.ds(me, 1)] = far_out_b[pl.ds(me, 1)]

    remote(idx2, idx3, sems.at[8], sems.at[9], partner).wait_recv()
    found = []
    for part in (idx2, idx3):
        listed = part[...].reshape(2 * area, peers)
        found.append(
            jnp.sum(jnp.where(iota(listed.shape, 1) == me, listed, 0), axis=1, keepdims=True)
        )
    found = jnp.concatenate(found, axis=0)
    slots_t = []
    for slot in range(2):
        there = iota((4 * area, peers), 0) == key * 2 + slot
        asked = jnp.sum(jnp.where(there, found, 0), axis=0, keepdims=True)
        line = jnp.zeros_like(asked)
        for c in range(coarse_count):
            line = jnp.where(asked == c, coarse[c], line)
        slots_t.append(line)
    sums = mm(onehot_t[ext : ext + own, :], dpre[...]).astype(BF16)
    total = node_back + mm_nt(d_node, w_node[...]) + mm_nt(sums, w_send[...])
    sums = mm(onehot_t[send_pad : send_pad + own, :], dpre[...]).astype(BF16)
    total = total + mm_nt(sums, w_recv[...])

    def finish(step, carry):
        at = pl.ds(pl.multiple_of(step * rows, rows), rows)
        grad = edge_cot[at, :].astype(F32) + mm_nt(dpre[at, :], w_edge[...])
        edge_grad[at, :] = grad.astype(BF16)
        return carry

    lax.fori_loop(0, steps, finish, 0)

    for k in range(near_count):
        near_b[k].wait_recv()
        mask = iota((own, near_rows), 0) == near_lists[k : k + 1, :]
        total = total + mm(hot(mask), near_in_b[k])
    remote(far_out_b.at[others], far_in_b.at[others], sems.at[10], sems.at[11], partner).wait_recv()
    pair = collect_rows(far_in_b, wide, peers, width)
    for s in range(2):
        mask = iota((own, peers), 0) == slots_t[s]
        total = total + mm(hot(mask), pair[s].astype(BF16))
    node_grad[...] = total.astype(BF16)
    for copy in near:
        copy.wait_send()
    for copy in near_b:
        copy.wait_send()
    remote(row1.at[fewer], row1.at[fewer], sems.at[0], sems.at[1], partner).wait_send()
    remote(idx1.at[fewer], idx1.at[fewer], sems.at[2], sems.at[3], partner).wait_send()
    for copy in hops:
        copy.wait_send()
    remote(row2, row3, sems.at[4], sems.at[5], partner).wait_send()
    remote(idx2.at[fewer], idx2.at[fewer], sems.at[6], sems.at[7], partner).wait_send()
    remote(idx2, idx3, sems.at[8], sems.at[9], partner).wait_send()
    remote(far_out_b.at[others], far_in_b.at[others], sems.at[10], sems.at[11], partner).wait_send()


def place_kernel(a, b, c, d, a_out, b_out, c_out, d_out, sems):
    pairs = ((b, b_out), (d, d_out), (a, a_out), (c, c_out))
    copies = [pltpu.make_async_copy(x, y, sems.at[i]) for i, (x, y) in enumerate(pairs)]
    for copy in copies:
        copy.start()
    for copy in copies:
        copy.wait()


VM = pl.BlockSpec(memory_space=pltpu.VMEM)
SM = pl.BlockSpec(memory_space=pltpu.SMEM)
HBM = pl.BlockSpec(memory_space=pltpu.HBM)
ANY = pl.BlockSpec(memory_space=pl.ANY)
DMA = pltpu.SemaphoreType.DMA
ROWS = 512


def local(
    nodes, edges, node_cot, edge_cot, w_edge, w_send, w_recv, edge_bias, w_edge_out,
    edge_out_bias, edge_gain, w_node, w_agg, node_bias, w_node_out, node_out_bias, node_gain,
    send_slots, recv_slots, neighbour_send_lists, coarse_rows, far_lists, block_count,
):
    own, width = nodes.shape
    total_edges = edges.shape[0]
    peers = lax.axis_size("patch")
    near_count, near_rows = neighbour_send_lists.shape
    near_total = near_count * near_rows
    ext = near_total + 2 * peers
    unit_rows = 2 * width // LANES
    send_pad = -(-(ext + own) // LANES) * LANES
    recv_pad = -(-own // LANES) * LANES
    flat = lambda v: v.reshape(1, -1)
    near_b = pltpu.VMEM((near_count, near_rows, width), BF16)
    side, coarse = side_of(peers), coarse_rows.shape[0]
    far_b = pltpu.VMEM((peers, unit_rows, LANES), BF16)
    node_b = pltpu.VMEM((own, width), BF16)
    slot_b = pltpu.VMEM((total_edges // LANES, LANES), jnp.int32)
    weight = pltpu.VMEM((width, width), BF16)
    edge_b = pltpu.VMEM((total_edges, width), BF16)
    edge_f = pltpu.VMEM((total_edges, width), F32)
    shapes = tuple(
        jax.ShapeDtypeStruct((n, width), BF16) for n in (own, total_edges, own, total_edges)
    )
    results = pl.pallas_call(
        functools.partial(layer_kernel, ROWS, peers),
        name="layer",
        out_shape=tuple(pltpu.VMEM(v.shape, v.dtype) for v in shapes),
        in_specs=[SM] * 2 + [HBM] * 21,
        out_specs=(VM,) * 4,
        scratch_shapes=[near_b] * 4
        + [pltpu.VMEM((peers * unit_rows, LANES), F32)] + [far_b] * 2
        + [
            pltpu.VMEM((side, coarse, width), BF16),
            pltpu.VMEM((side, side, coarse, width), BF16),
            pltpu.VMEM((side, side, coarse, width), BF16),
            pltpu.VMEM((side, 2, peers), jnp.int32),
            pltpu.VMEM((side, side, 2, peers), jnp.int32),
            pltpu.VMEM((side, side, 2, peers), jnp.int32),
            pltpu.VMEM((2 * peers, 2 * side * side * coarse), BF16),
        ]
        + [
            node_b, pltpu.VMEM(neighbour_send_lists.shape, jnp.int32), pltpu.VMEM((1, 2, peers), jnp.int32),
            slot_b, slot_b, node_b,
        ]
        + [pltpu.VMEM((1, width), F32)] * 6
        + [edge_b] * 2 + [weight] * 7
        + [
            pltpu.VMEM((send_pad + recv_pad, width), BF16),
            pltpu.VMEM((total_edges, send_pad + recv_pad), BF16),
            pltpu.VMEM((send_pad + recv_pad, total_edges), BF16),
            edge_f, edge_f,
            pltpu.VMEM((total_edges, LANES), F32),
            edge_b, edge_b,
            pltpu.VMEM((recv_pad, width), BF16),
        ]
        + [DMA((near_count,))] * 4 + [DMA((12,)), DMA((2, side - 1)), DMA((21,))],
        compiler_params=pltpu.CompilerParams(
            collective_id=0, has_side_effects=True, vmem_limit_bytes=VMEM_LIMIT
        ),
    )(
        coarse_rows, block_count, nodes, neighbour_send_lists, far_lists.transpose(0, 2, 1),
        send_slots.reshape(-1, LANES), recv_slots.reshape(-1, LANES), node_cot,
        flat(edge_bias), flat(edge_out_bias), flat(edge_gain), flat(node_bias),
        flat(node_out_bias), flat(node_gain),
        edges, edge_cot, w_edge, w_send, w_recv, w_edge_out, w_node, w_agg, w_node_out,
    )
    return pl.pallas_call(
        place_kernel,
        name="place",
        out_shape=shapes,
        in_specs=[VM] * 4,
        out_specs=(ANY,) * 4,
        scratch_shapes=[DMA((4,))],
        compiler_params=pltpu.CompilerParams(vmem_limit_bytes=8 << 20),
    )(*results)


def solution(mesh):
    both = P(("groups", "patch"), None)
    placed = (both,) * 4 + (P(),) * 13 + (
        P("patch"), P("patch"), P("patch", None), P("patch"), P("patch", None, None), P("patch"),
    )
    return jax.shard_map(
        local, mesh=mesh, in_specs=placed, out_specs=(both,) * 4, check_vma=False
    )
```

```python
import functools
import math

import jax
import jax.numpy as jnp
from jax import lax
from jax.experimental import pallas as pl
from jax.experimental.pallas import tpu as pltpu
from jax.sharding import PartitionSpec as P

BLOCK = 128
LANES = 128
MESH = pl.DeviceIdType.MESH
F32 = jnp.float32
BF16 = jnp.bfloat16
VMEM_LIMIT = 60 << 20


def mm(a, b):
    return lax.dot_general(a, b, (((1,), (0,)), ((), ())), preferred_element_type=F32)


def mm_nt(a, b):
    return lax.dot_general(a, b, (((1,), (1,)), ((), ())), preferred_element_type=F32)


def mm_tn(a, b):
    return lax.dot_general(a, b, (((0,), (0,)), ((), ())), preferred_element_type=F32)


def iota(shape, dim):
    return lax.broadcasted_iota(jnp.int32, shape, dim)


def hot(mask):
    return jnp.where(mask, 1.0, 0.0).astype(BF16)


def offsets_of(count):
    return [(index // 2 + 1) * (1 - 2 * (index % 2)) for index in range(count)]


def side_of(peers):
    return math.isqrt(peers // 2)


def far_first(side):
    half = side // 2
    return sorted(range(1, side), key=lambda k: -min(k, side - k)) if half else []


def place_of(me, side):
    core = lax.rem(me, 2)
    line = lax.rem(lax.div(me, 2), side)
    return lax.div(me, 2 * side), line, core


def wrapped(value, side):
    return jnp.where(value >= side, value - side, value)


def every_peer(me, side, body):
    x, y, core = place_of(me, side)
    within = [(oy, oc) for oy in far_first(side) + [0] for oc in (0, 1)]
    lines = {oy: 2 * wrapped(y + oy, side) for oy in range(side)}
    cores = (core, 1 - core)

    def step(i, carry):
        away = lax.div(i + 1, 2) * (1 - 2 * lax.rem(i, 2))
        row = wrapped(x + side // 2 + away, side) * (2 * side)
        for oy, oc in within:
            body(row + lines[oy] + cores[oc])
        return carry

    lax.fori_loop(0, side - 1, step, 0)
    for oy, oc in within[:-2] + [(0, 1)]:
        body(x * (2 * side) + lines[oy] + cores[oc])


def remote(src, dst, send, recv, peer):
    return pltpu.make_async_remote_copy(
        src_ref=src, dst_ref=dst, send_sem=send, recv_sem=recv,
        device_id={"patch": peer}, device_id_type=MESH,
    )


def spread_rows(pair, wide, packed, peers):
    parts = pair[0].shape[1] // LANES
    unit = 2 * parts
    for slot in range(2):
        for part in range(parts):
            wide[pl.ds(2 * part + slot, peers, stride=unit), :] = pair[slot][
                :, part * LANES : (part + 1) * LANES
            ]
    packed[...] = wide[...].reshape(peers, unit, LANES).astype(BF16)


def collect_rows(packed, wide, peers, width):
    parts = width // LANES
    unit = 2 * parts
    wide[...] = packed[...].astype(F32).reshape(peers * unit, LANES)
    pair = []
    for slot in range(2):
        pieces = [
            wide[pl.ds(2 * part + slot, peers, stride=unit), :] for part in range(parts)
        ]
        pair.append(jnp.concatenate(pieces, axis=1))
    return pair


def normal_stats(values):
    center = values - jnp.mean(values, axis=-1, keepdims=True)
    spread = jnp.mean(center * center, axis=-1, keepdims=True)
    inv = lax.rsqrt(spread + 1e-05)
    return center * inv, inv


def normal_back(grad, unit, inv):
    along = jnp.mean(grad * unit, axis=-1, keepdims=True)
    return inv * (grad - jnp.mean(grad, axis=-1, keepdims=True) - unit * along)


def silu_both(half):
    t = jnp.tanh(half)
    out = half + half * t
    return out, (1.0 + t) + out * (1.0 - t)


def layer_kernel(
    rows, peers,
    counts,
    nodes_h, near_lists_h, far_lists_h, coarse_h, send_rows_h, recv_rows_h, node_cot_h,
    edge_bias_h, edge_out_bias_h, edge_gain_h, node_bias_h, node_out_bias_h, node_gain_h,
    edges_h, edge_cot_h, w_edge_h, w_send_h, w_recv_h, w_edge_out_h, w_node_h, w_agg_h, w_node_out_h,
    new_nodes, new_edges, node_grad, edge_grad,
    near_out, near_in, near_out_b, near_in_b, wide, far_out_b, far_in_b,
    row1, row2, row3, idx1, idx2, idx3, picks,
    nodes, near_lists, far_lists, coarse, send_rows, recv_rows, node_cot,
    edge_bias, edge_out_bias, edge_gain, node_bias, node_out_bias, node_gain,
    edges, edge_cot, w_edge, w_send, w_recv, w_edge_out, w_node, w_agg, w_node_out,
    w_edge_out_t, w_node_out_t, w_agg_t, w_send_t,
    proj, onehot, onehot_t, slope, unit, invs, sent, dpre, dagg,
    near_send, near_recv, near_send_b, near_recv_b, sems, hop_sems, in_sems,
):
    me = lax.axis_index("patch")
    own, width = nodes.shape
    total_edges = edges.shape[0]
    near_count, near_rows = near_lists.shape
    near_total = near_count * near_rows
    ext = near_total + 2 * peers
    send_pad = -(-(ext + own) // LANES) * LANES
    recv_pad = -(-own // LANES) * LANES
    steps = total_edges // rows
    offsets = offsets_of(near_count)
    others = pl.ds(0, peers - 1)

    side = side_of(peers)
    x, y, core = place_of(me, side)
    first_step = jnp.where(core == 0, 2 * side, 2)
    second_step = jnp.where(core == 0, 2, 2 * side)
    first_at = jnp.where(core == 0, x, y)
    second_at = jnp.where(core == 0, y, x)
    partner = me + 1 - 2 * core
    order = far_first(side)
    first_peers = [me + (wrapped(first_at + k, side) - first_at) * first_step for k in order]
    second_peers = [me + (wrapped(second_at + k, side) - second_at) * second_step for k in order]
    near_peers = [lax.rem(me + o + peers, peers) for o in offsets]
    barrier = pltpu.get_barrier_semaphore()
    known = first_peers + second_peers + near_peers + [partner]
    for peer in known:
        pl.semaphore_signal(barrier, inc=1, device_id={"patch": peer}, device_id_type=MESH)
    moves = [
        (nodes_h, nodes), (near_lists_h, near_lists), (far_lists_h, far_lists), (coarse_h, coarse),
        (send_rows_h, send_rows), (recv_rows_h, recv_rows), (edge_bias_h, edge_bias),
        (edge_out_bias_h, edge_out_bias), (edge_gain_h, edge_gain), (node_bias_h, node_bias),
        (node_out_bias_h, node_out_bias), (node_gain_h, node_gain), (node_cot_h, node_cot),
        (w_send_h, w_send), (w_recv_h, w_recv), (edges_h, edges), (w_edge_h, w_edge),
        (w_edge_out_h, w_edge_out), (w_agg_h, w_agg), (w_node_h, w_node),
        (w_node_out_h, w_node_out), (edge_cot_h, edge_cot),
    ]
    copies = [pltpu.make_async_copy(a, b, in_sems.at[i]) for i, (a, b) in enumerate(moves)]
    for copy in copies:
        copy.start()
    first_big = len(copies) - 9

    for i in range(4):
        copies[i].wait()
    coarse_count = coarse.shape[0]
    chosen = jnp.zeros((coarse_count, own), jnp.int32)
    for c in range(coarse_count):
        chosen = jnp.where(iota(chosen.shape, 0) == c, coarse[c], chosen)
    rows_out = mm(hot(iota(chosen.shape, 1) == chosen), nodes[...]).astype(BF16)
    row1[pl.ds(first_at, 1)] = rows_out.reshape(1, coarse_count, width)
    idx1[pl.ds(first_at, 1)] = far_lists[...]

    pl.semaphore_wait(barrier, len(known))
    mine = row1.at[first_at]
    for peer in first_peers:
        remote(mine, mine, sems.at[0], sems.at[1], peer).start()
    for k in range(near_count):
        mask = iota((own, near_rows), 0) == near_lists[k : k + 1, :]
        near_out[k] = mm_tn(hot(mask), nodes[...]).astype(BF16)
    near = []
    for k in range(near_count):
        copy = remote(near_out.at[k], near_in.at[k], near_send.at[k], near_recv.at[k], near_peers[k])
        copy.start()
        near.append(copy)
    mine = idx1.at[first_at]
    for peer in first_peers:
        remote(mine, mine, sems.at[2], sems.at[3], peer).start()

    for i in range(4, first_big):
        copies[i].wait()
    copies = copies[first_big:]
    raw = send_rows[...]
    far = raw - own - near_total
    address = jnp.where(
        raw < own, raw + ext,
        jnp.where(raw < own + near_total, raw - own,
                  near_total + jnp.bitwise_and(far, 1) * peers + lax.shift_right_arithmetic(far, 1)),
    )
    target = recv_rows[...]
    lane = iota((LANES, LANES), 1)
    for g in range(total_edges // LANES):
        line = address[g : g + 1, :]
        goal = target[g : g + 1, :]
        span = slice(g * LANES, (g + 1) * LANES)
        onehot_t[0:send_pad, span] = hot(iota((send_pad, LANES), 0) == line)
        onehot_t[send_pad:, span] = hot(iota((recv_pad, LANES), 0) == goal)
        line_col = jnp.broadcast_to(line, (LANES, LANES)).T
        goal_col = jnp.broadcast_to(goal, (LANES, LANES)).T
        for c in range(send_pad // LANES):
            onehot[span, c * LANES : (c + 1) * LANES] = hot(line_col == lane + c * LANES)
        for c in range(recv_pad // LANES):
            onehot[span, send_pad + c * LANES : send_pad + (c + 1) * LANES] = hot(
                goal_col == lane + c * LANES
            )
    area = side * side
    q = iota((1, peers), 1)
    q_core = jnp.bitwise_and(q, 1)
    q_chip = lax.shift_right_logical(q, 1)
    q_x = q_chip // side
    q_y = q_chip - q_x * side
    key = jnp.where(q_core == 0, q_y * side + q_x, q_x * side + q_y)
    key = key + jnp.where(q_core == core, 0, area)
    for slot in range(2):
        spot = key * coarse_count + far_lists[0, slot : slot + 1, :]
        spot_col = jnp.broadcast_to(spot, (LANES, peers)).T
        picks[slot * peers : (slot + 1) * peers, :] = hot(
            iota((peers, 2 * area * coarse_count), 1) == spot_col[:, 0:1]
        )

    fewer = pl.ds(0, side - 1)
    remote(row1.at[fewer], row1.at[fewer], sems.at[0], sems.at[1], partner).wait_recv()
    hops = []
    for i, peer in enumerate(second_peers):
        copy = remote(row1, row2.at[second_at], hop_sems.at[0, i], hop_sems.at[1, i], peer)
        copy.start()
        hops.append(copy)
    remote(row1, row3.at[second_at], sems.at[4], sems.at[5], partner).start()
    row2[pl.ds(second_at, 1)] = row1[...].reshape(1, side, coarse_count, width)
    remote(idx1.at[fewer], idx1.at[fewer], sems.at[2], sems.at[3], partner).wait_recv()
    for peer in second_peers:
        remote(idx1, idx2.at[second_at], sems.at[6], sems.at[7], peer).start()
    idx2[pl.ds(second_at, 1)] = idx1[...].reshape(1, side, 2, peers)

    proj[ext + own : send_pad, :] = jnp.zeros((send_pad - ext - own, width), BF16)
    proj[send_pad + own :, :] = jnp.zeros((recv_pad - own, width), BF16)
    dagg[own:, :] = jnp.zeros((recv_pad - own, width), BF16)
    copies[0].wait()
    proj[ext : ext + own, :] = mm(nodes[...], w_send[...]).astype(BF16)
    copies[1].wait()
    proj[send_pad : send_pad + own, :] = mm(nodes[...], w_recv[...]).astype(BF16)
    copies[2].wait()
    copies[3].wait()
    for copy in near:
        copy.wait_recv()
    proj[0:near_total, :] = mm(near_in[...].reshape(near_total, width), w_send[...]).astype(BF16)

    def ahead(step, carry):
        at = pl.ds(pl.multiple_of(step * rows, rows), rows)
        slope[at, :] = 0.5 * (
            mm(edges[at, :], w_edge[...])
            + mm(onehot[at, 0:near_total], proj[0:near_total, :])
            + mm(onehot[at, ext:], proj[ext:, :])
            + edge_bias[...]
        )
        return carry

    lax.fori_loop(0, steps, ahead, 0)

    for i in reversed(range(len(order))):
        hops[i].wait_recv()
        origin = wrapped(second_at + side - order[i], side)
        remote(row2.at[origin], row3.at[origin], sems.at[4], sems.at[5], partner).start()
    remote(idx2.at[fewer], idx2.at[fewer], sems.at[6], sems.at[7], partner).wait_recv()
    remote(idx2, idx3, sems.at[8], sems.at[9], partner).start()
    for i in (4, 5, 6, 7, 8):
        copies[i].wait()
    node_pre = mm(nodes[...], w_node[...]) + node_bias[...]
    node_back = node_cot[...].astype(F32)
    for w, turned in ((w_edge_out, w_edge_out_t), (w_node_out, w_node_out_t), (w_agg, w_agg_t), (w_send, w_send_t)):
        turned[...] = w[...].T
    live_rows = counts[0] * BLOCK

    half = area * coarse_count
    mine_rows = mm(picks[:, 0:half], row2[...].reshape(half, width))
    remote(row2, row3, sems.at[4], sems.at[5], partner).wait_recv()
    far_rows = mine_rows + mm(picks[:, half:], row3[...].reshape(half, width))
    proj[near_total:ext, :] = (0.5 * mm(far_rows.astype(BF16), w_send[...])).astype(BF16)

    gathered = []
    for step in range(steps):
        at = slice(step * rows, (step + 1) * rows)
        half_pre = slope[at, :] + mm(onehot[at, near_total:ext], proj[near_total:ext, :])
        hidden, rise = silu_both(half_pre)
        slope[at, :] = rise
        out = mm(hidden.astype(BF16), w_edge_out[...]) + edge_out_bias[...]
        center = out - jnp.mean(out, axis=-1, keepdims=True)
        inv = lax.rsqrt(jnp.mean(center * center, axis=-1, keepdims=True) + 1e-05)
        inv = jnp.where(iota((rows, 1), 0) + step * rows < live_rows, inv, 0.0)
        normed = center * inv
        unit[at, :] = normed
        invs[at, :] = jnp.broadcast_to(0.5 * inv, (rows, LANES))
        sent[at, :] = (edge_gain[...] * normed).astype(BF16)
        gathered.append(mm(onehot_t[send_pad : send_pad + own, at], sent[at, :]))

    aggregate = sum(gathered[1:], gathered[0]).astype(BF16)
    hidden, rise = silu_both(0.5 * (node_pre + mm(aggregate, w_agg[...])))
    out = mm(hidden.astype(BF16), w_node_out[...]) + node_out_bias[...]
    normed, inv = normal_stats(out)
    new_nodes[...] = (nodes[...].astype(F32) + node_gain[...] * normed).astype(BF16)
    d_out = normal_back(node_gain[...] * node_back, normed, 0.5 * inv).astype(BF16)
    d_node = (mm(d_out, w_node_out_t[...]) * rise).astype(BF16)
    dagg[0:own, :] = mm(d_node, w_agg_t[...]).astype(BF16)

    gathered = []
    for step in range(steps):
        at = slice(step * rows, (step + 1) * rows)
        d_message = edge_cot[at, :].astype(F32) + mm(onehot[at, send_pad:], dagg[...])
        d_out = normal_back(edge_gain[...] * d_message, unit[at, :], invs[at, 0:1]).astype(BF16)
        dpre[at, :] = (mm(d_out, w_edge_out_t[...]) * slope[at, :]).astype(BF16)
        gathered.append(mm(onehot_t[0:ext, at], dpre[at, :]))

    sums = sum(gathered[1:], gathered[0]).astype(BF16)
    back = mm(sums, w_send_t[...])
    near_out_b[...] = back[0:near_total, :].astype(BF16).reshape(near_count, near_rows, width)
    pair = [back[near_total + s * peers : near_total + (s + 1) * peers, :] for s in range(2)]
    spread_rows(pair, wide, far_out_b, peers)
    every_peer(
        me, side,
        lambda peer: remote(
            far_out_b.at[peer], far_in_b.at[me], sems.at[10], sems.at[11], peer
        ).start(),
    )
    near_b = []
    for k in range(near_count):
        copy = remote(
            near_out_b.at[k], near_in_b.at[k], near_send_b.at[k], near_recv_b.at[k],
            lax.rem(me - offsets[k] + peers, peers),
        )
        copy.start()
        near_b.append(copy)
    far_in_b[pl.ds(me, 1)] = far_out_b[pl.ds(me, 1)]

    remote(idx2, idx3, sems.at[8], sems.at[9], partner).wait_recv()
    found = []
    for part in (idx2, idx3):
        listed = part[...].reshape(2 * area, peers)
        found.append(
            jnp.sum(jnp.where(iota(listed.shape, 1) == me, listed, 0), axis=1, keepdims=True)
        )
    found = jnp.concatenate(found, axis=0)
    slots_t = []
    for slot in range(2):
        there = iota((4 * area, peers), 0) == key * 2 + slot
        asked = jnp.sum(jnp.where(there, found, 0), axis=0, keepdims=True)
        line = jnp.zeros_like(asked)
        for c in range(coarse_count):
            line = jnp.where(asked == c, coarse[c], line)
        slots_t.append(line)
    sums = mm(onehot_t[ext : ext + own, :], dpre[...]).astype(BF16)
    total = node_back + mm_nt(d_node, w_node[...]) + mm(sums, w_send_t[...])
    sums = mm(onehot_t[send_pad : send_pad + own, :], dpre[...]).astype(BF16)
    total = total + mm_nt(sums, w_recv[...])

    def finish(step, carry):
        at = pl.ds(pl.multiple_of(step * rows, rows), rows)
        grad = edge_cot[at, :].astype(F32) + mm_nt(dpre[at, :], w_edge[...])
        edge_grad[at, :] = grad.astype(BF16)
        new_edges[at, :] = (edges[at, :].astype(F32) + edge_gain[...] * unit[at, :]).astype(BF16)
        return carry

    lax.fori_loop(0, steps, finish, 0)

    for k in range(near_count):
        near_b[k].wait_recv()
        mask = iota((own, near_rows), 0) == near_lists[k : k + 1, :]
        total = total + mm(hot(mask), near_in_b[k])
    remote(far_out_b.at[others], far_in_b.at[others], sems.at[10], sems.at[11], partner).wait_recv()
    pair = collect_rows(far_in_b, wide, peers, width)
    for s in range(2):
        mask = iota((own, peers), 0) == slots_t[s]
        total = total + mm(hot(mask), pair[s].astype(BF16))
    node_grad[...] = total.astype(BF16)
    for copy in near:
        copy.wait_send()
    for copy in near_b:
        copy.wait_send()
    remote(row1.at[fewer], row1.at[fewer], sems.at[0], sems.at[1], partner).wait_send()
    remote(idx1.at[fewer], idx1.at[fewer], sems.at[2], sems.at[3], partner).wait_send()
    for copy in hops:
        copy.wait_send()
    remote(row2, row3, sems.at[4], sems.at[5], partner).wait_send()
    remote(idx2.at[fewer], idx2.at[fewer], sems.at[6], sems.at[7], partner).wait_send()
    remote(idx2, idx3, sems.at[8], sems.at[9], partner).wait_send()
    remote(far_out_b.at[others], far_in_b.at[others], sems.at[10], sems.at[11], partner).wait_send()


def place_kernel(a, b, c, d, a_out, b_out, c_out, d_out, sems):
    pairs = ((b, b_out), (d, d_out), (a, a_out), (c, c_out))
    copies = [pltpu.make_async_copy(x, y, sems.at[i]) for i, (x, y) in enumerate(pairs)]
    for copy in copies:
        copy.start()
    for copy in copies:
        copy.wait()


VM = pl.BlockSpec(memory_space=pltpu.VMEM)
SM = pl.BlockSpec(memory_space=pltpu.SMEM)
HBM = pl.BlockSpec(memory_space=pltpu.HBM)
ANY = pl.BlockSpec(memory_space=pl.ANY)
DMA = pltpu.SemaphoreType.DMA
ROWS = 512


def local(
    nodes, edges, node_cot, edge_cot, w_edge, w_send, w_recv, edge_bias, w_edge_out,
    edge_out_bias, edge_gain, w_node, w_agg, node_bias, w_node_out, node_out_bias, node_gain,
    send_slots, recv_slots, neighbour_send_lists, coarse_rows, far_lists, block_count,
):
    own, width = nodes.shape
    total_edges = edges.shape[0]
    peers = lax.axis_size("patch")
    near_count, near_rows = neighbour_send_lists.shape
    near_total = near_count * near_rows
    ext = near_total + 2 * peers
    unit_rows = 2 * width // LANES
    send_pad = -(-(ext + own) // LANES) * LANES
    recv_pad = -(-own // LANES) * LANES
    flat = lambda v: v.reshape(1, -1)
    near_b = pltpu.VMEM((near_count, near_rows, width), BF16)
    side, coarse = side_of(peers), coarse_rows.shape[0]
    far_b = pltpu.VMEM((peers, unit_rows, LANES), BF16)
    node_b = pltpu.VMEM((own, width), BF16)
    slot_b = pltpu.VMEM((total_edges // LANES, LANES), jnp.int32)
    weight = pltpu.VMEM((width, width), BF16)
    edge_b = pltpu.VMEM((total_edges, width), BF16)
    edge_f = pltpu.VMEM((total_edges, width), F32)
    shapes = tuple(
        jax.ShapeDtypeStruct((n, width), BF16) for n in (own, total_edges, own, total_edges)
    )
    results = pl.pallas_call(
        functools.partial(layer_kernel, ROWS, peers),
        name="layer",
        out_shape=tuple(pltpu.VMEM(v.shape, v.dtype) for v in shapes),
        in_specs=[SM] + [HBM] * 22,
        out_specs=(VM,) * 4,
        scratch_shapes=[near_b] * 4
        + [pltpu.VMEM((peers * unit_rows, LANES), F32)] + [far_b] * 2
        + [
            pltpu.VMEM((side, coarse, width), BF16),
            pltpu.VMEM((side, side, coarse, width), BF16),
            pltpu.VMEM((side, side, coarse, width), BF16),
            pltpu.VMEM((side, 2, peers), jnp.int32),
            pltpu.VMEM((side, side, 2, peers), jnp.int32),
            pltpu.VMEM((side, side, 2, peers), jnp.int32),
            pltpu.VMEM((2 * peers, 2 * side * side * coarse), BF16),
        ]
        + [
            node_b, pltpu.VMEM(neighbour_send_lists.shape, jnp.int32), pltpu.VMEM((1, 2, peers), jnp.int32),
            pltpu.SMEM(coarse_rows.shape, jnp.int32), slot_b, slot_b, node_b,
        ]
        + [pltpu.VMEM((1, width), F32)] * 6
        + [edge_b] * 2 + [weight] * 11
        + [
            pltpu.VMEM((send_pad + recv_pad, width), BF16),
            pltpu.VMEM((total_edges, send_pad + recv_pad), BF16),
            pltpu.VMEM((send_pad + recv_pad, total_edges), BF16),
            edge_f, edge_f,
            pltpu.VMEM((total_edges, LANES), F32),
            edge_b, edge_b,
            pltpu.VMEM((recv_pad, width), BF16),
        ]
        + [DMA((near_count,))] * 4 + [DMA((12,)), DMA((2, side - 1)), DMA((22,))],
        compiler_params=pltpu.CompilerParams(
            collective_id=0, has_side_effects=True, vmem_limit_bytes=VMEM_LIMIT
        ),
    )(
        block_count, nodes, neighbour_send_lists, far_lists.transpose(0, 2, 1), coarse_rows,
        send_slots.reshape(-1, LANES), recv_slots.reshape(-1, LANES), node_cot,
        flat(edge_bias), flat(edge_out_bias), flat(edge_gain), flat(node_bias),
        flat(node_out_bias), flat(node_gain),
        edges, edge_cot, w_edge, w_send, w_recv, w_edge_out, w_node, w_agg, w_node_out,
    )
    return pl.pallas_call(
        place_kernel,
        name="place",
        out_shape=shapes,
        in_specs=[VM] * 4,
        out_specs=(ANY,) * 4,
        scratch_shapes=[DMA((4,))],
        compiler_params=pltpu.CompilerParams(vmem_limit_bytes=8 << 20),
    )(*results)


def solution(mesh):
    both = P(("groups", "patch"), None)
    placed = (both,) * 4 + (P(),) * 13 + (
        P("patch"), P("patch"), P("patch", None), P("patch"), P("patch", None, None), P("patch"),
    )
    return jax.shard_map(
        local, mesh=mesh, in_specs=placed, out_specs=(both,) * 4, check_vma=False
    )
```

```python
import functools
import math

import jax
import jax.numpy as jnp
from jax import lax
from jax.experimental import pallas as pl
from jax.experimental.pallas import tpu as pltpu
from jax.sharding import PartitionSpec as P

BLOCK = 128
LANES = 128
MESH = pl.DeviceIdType.MESH
F32 = jnp.float32
BF16 = jnp.bfloat16
VMEM_LIMIT = 60 << 20


def mm(a, b):
    return lax.dot_general(a, b, (((1,), (0,)), ((), ())), preferred_element_type=F32)


def mm_nt(a, b):
    return lax.dot_general(a, b, (((1,), (1,)), ((), ())), preferred_element_type=F32)


def mm_tn(a, b):
    return lax.dot_general(a, b, (((0,), (0,)), ((), ())), preferred_element_type=F32)


def iota(shape, dim):
    return lax.broadcasted_iota(jnp.int32, shape, dim)


def hot(mask):
    return jnp.where(mask, 1.0, 0.0).astype(BF16)


def offsets_of(count):
    return [(index // 2 + 1) * (1 - 2 * (index % 2)) for index in range(count)]


def side_of(peers):
    return math.isqrt(peers // 2)


def far_first(side):
    half = side // 2
    return sorted(range(1, side), key=lambda k: -min(k, side - k)) if half else []


def place_of(me, side):
    core = lax.rem(me, 2)
    line = lax.rem(lax.div(me, 2), side)
    return lax.div(me, 2 * side), line, core


def wrapped(value, side):
    return jnp.where(value >= side, value - side, value)


def every_peer(me, side, body):
    x, y, core = place_of(me, side)
    within = [(oy, oc) for oy in far_first(side) + [0] for oc in (0, 1)]
    lines = {oy: 2 * wrapped(y + oy, side) for oy in range(side)}
    cores = (core, 1 - core)

    def step(i, carry):
        away = lax.div(i + 1, 2) * (1 - 2 * lax.rem(i, 2))
        row = wrapped(x + side // 2 + away, side) * (2 * side)
        for oy, oc in within:
            body(row + lines[oy] + cores[oc])
        return carry

    lax.fori_loop(0, side - 1, step, 0)
    for oy, oc in within[:-2] + [(0, 1)]:
        body(x * (2 * side) + lines[oy] + cores[oc])


def remote(src, dst, send, recv, peer):
    return pltpu.make_async_remote_copy(
        src_ref=src, dst_ref=dst, send_sem=send, recv_sem=recv,
        device_id={"patch": peer}, device_id_type=MESH,
    )


def spread_rows(pair, wide, packed, peers):
    parts = pair[0].shape[1] // LANES
    unit = 2 * parts
    for slot in range(2):
        for part in range(parts):
            wide[pl.ds(2 * part + slot, peers, stride=unit), :] = pair[slot][
                :, part * LANES : (part + 1) * LANES
            ]
    packed[...] = wide[...].reshape(peers, unit, LANES).astype(BF16)


def collect_rows(packed, wide, peers, width):
    parts = width // LANES
    unit = 2 * parts
    wide[...] = packed[...].astype(F32).reshape(peers * unit, LANES)
    pair = []
    for slot in range(2):
        pieces = [
            wide[pl.ds(2 * part + slot, peers, stride=unit), :] for part in range(parts)
        ]
        pair.append(jnp.concatenate(pieces, axis=1))
    return pair


def normal_stats(values):
    center = values - jnp.mean(values, axis=-1, keepdims=True)
    spread = jnp.mean(center * center, axis=-1, keepdims=True)
    inv = lax.rsqrt(spread + 1e-05)
    return center * inv, inv


def normal_back(grad, unit, inv):
    along = jnp.mean(grad * unit, axis=-1, keepdims=True)
    return inv * (grad - jnp.mean(grad, axis=-1, keepdims=True) - unit * along)


def silu_both(half):
    t = jnp.tanh(half)
    out = half + half * t
    return out, (1.0 + t) + out * (1.0 - t)


def layer_kernel(
    rows, peers,
    counts,
    nodes_h, near_lists_h, far_lists_h, coarse_h, send_rows_h, recv_rows_h, node_cot_h,
    edge_bias_h, edge_out_bias_h, edge_gain_h, node_bias_h, node_out_bias_h, node_gain_h,
    edges_h, edge_cot_h, w_edge_h, w_send_h, w_recv_h, w_edge_out_h, w_node_h, w_agg_h, w_node_out_h,
    new_nodes, new_edges, node_grad, edge_grad,
    near_out, near_in, near_out_b, near_in_b, wide, far_out_b, far_in_b,
    row1, row2, row3, idx1, idx2, idx3, picks,
    nodes, near_lists, far_lists, coarse, send_rows, recv_rows, node_cot,
    edge_bias, edge_out_bias, edge_gain, node_bias, node_out_bias, node_gain,
    edges, edge_cot, w_edge, w_send, w_recv, w_edge_out, w_node, w_agg, w_node_out,
    w_edge_out_t, w_node_out_t, w_agg_t, w_send_t,
    proj, onehot, onehot_t, slope, unit, invs, sent, dpre, dagg,
    near_send, near_recv, near_send_b, near_recv_b, sems, hop_sems, in_sems,
):
    me = lax.axis_index("patch")
    own, width = nodes.shape
    total_edges = edges.shape[0]
    near_count, near_rows = near_lists.shape
    near_total = near_count * near_rows
    ext = near_total + 2 * peers
    send_pad = -(-(ext + own) // LANES) * LANES
    recv_pad = -(-own // LANES) * LANES
    steps = total_edges // rows
    offsets = offsets_of(near_count)
    others = pl.ds(0, peers - 1)

    side = side_of(peers)
    x, y, core = place_of(me, side)
    first_step = jnp.where(core == 0, 2 * side, 2)
    second_step = jnp.where(core == 0, 2, 2 * side)
    first_at = jnp.where(core == 0, x, y)
    second_at = jnp.where(core == 0, y, x)
    partner = me + 1 - 2 * core
    order = far_first(side)
    first_peers = [me + (wrapped(first_at + k, side) - first_at) * first_step for k in order]
    second_peers = [me + (wrapped(second_at + k, side) - second_at) * second_step for k in order]
    near_peers = [lax.rem(me + o + peers, peers) for o in offsets]
    barrier = pltpu.get_barrier_semaphore()
    known = first_peers + second_peers + near_peers + [partner]
    for peer in known:
        pl.semaphore_signal(barrier, inc=1, device_id={"patch": peer}, device_id_type=MESH)
    moves = [
        (nodes_h, nodes), (near_lists_h, near_lists), (far_lists_h, far_lists), (coarse_h, coarse),
        (send_rows_h, send_rows), (recv_rows_h, recv_rows), (edge_bias_h, edge_bias),
        (edge_out_bias_h, edge_out_bias), (edge_gain_h, edge_gain), (node_bias_h, node_bias),
        (node_out_bias_h, node_out_bias), (node_gain_h, node_gain), (node_cot_h, node_cot),
        (w_send_h, w_send), (w_recv_h, w_recv), (edges_h, edges), (w_edge_h, w_edge),
        (w_edge_out_h, w_edge_out), (w_agg_h, w_agg), (w_node_h, w_node),
        (w_node_out_h, w_node_out), (edge_cot_h, edge_cot),
    ]
    copies = [pltpu.make_async_copy(a, b, in_sems.at[i]) for i, (a, b) in enumerate(moves)]
    first_big = len(copies) - 9
    for copy in copies[:4]:
        copy.start()

    for i in range(4):
        copies[i].wait()
    coarse_count = coarse.shape[0]
    chosen = jnp.zeros((coarse_count, own), jnp.int32)
    for c in range(coarse_count):
        chosen = jnp.where(iota(chosen.shape, 0) == c, coarse[c], chosen)
    rows_out = mm(hot(iota(chosen.shape, 1) == chosen), nodes[...]).astype(BF16)
    row1[pl.ds(first_at, 1)] = rows_out.reshape(1, coarse_count, width)
    idx1[pl.ds(first_at, 1)] = far_lists[...]

    pl.semaphore_wait(barrier, len(known))
    mine = row1.at[first_at]
    for peer in first_peers:
        remote(mine, mine, sems.at[0], sems.at[1], peer).start()
    for copy in copies[4:]:
        copy.start()
    for k in range(near_count):
        mask = iota((own, near_rows), 0) == near_lists[k : k + 1, :]
        near_out[k] = mm_tn(hot(mask), nodes[...]).astype(BF16)
    near = []
    for k in range(near_count):
        copy = remote(near_out.at[k], near_in.at[k], near_send.at[k], near_recv.at[k], near_peers[k])
        copy.start()
        near.append(copy)
    mine = idx1.at[first_at]
    for peer in first_peers:
        remote(mine, mine, sems.at[2], sems.at[3], peer).start()

    for i in range(4, first_big):
        copies[i].wait()
    copies = copies[first_big:]
    raw = send_rows[...]
    far = raw - own - near_total
    address = jnp.where(
        raw < own, raw + ext,
        jnp.where(raw < own + near_total, raw - own,
                  near_total + jnp.bitwise_and(far, 1) * peers + lax.shift_right_arithmetic(far, 1)),
    )
    target = recv_rows[...]
    lane = iota((LANES, LANES), 1)
    for g in range(total_edges // LANES):
        line = address[g : g + 1, :]
        goal = target[g : g + 1, :]
        span = slice(g * LANES, (g + 1) * LANES)
        onehot_t[0:send_pad, span] = hot(iota((send_pad, LANES), 0) == line)
        onehot_t[send_pad:, span] = hot(iota((recv_pad, LANES), 0) == goal)
        line_col = jnp.broadcast_to(line, (LANES, LANES)).T
        goal_col = jnp.broadcast_to(goal, (LANES, LANES)).T
        for c in range(send_pad // LANES):
            onehot[span, c * LANES : (c + 1) * LANES] = hot(line_col == lane + c * LANES)
        for c in range(recv_pad // LANES):
            onehot[span, send_pad + c * LANES : send_pad + (c + 1) * LANES] = hot(
                goal_col == lane + c * LANES
            )
    area = side * side
    q = iota((1, peers), 1)
    q_core = jnp.bitwise_and(q, 1)
    q_chip = lax.shift_right_logical(q, 1)
    q_x = q_chip // side
    q_y = q_chip - q_x * side
    key = jnp.where(q_core == 0, q_y * side + q_x, q_x * side + q_y)
    key = key + jnp.where(q_core == core, 0, area)
    for slot in range(2):
        spot = key * coarse_count + far_lists[0, slot : slot + 1, :]
        spot_col = jnp.broadcast_to(spot, (LANES, peers)).T
        picks[slot * peers : (slot + 1) * peers, :] = hot(
            iota((peers, 2 * area * coarse_count), 1) == spot_col[:, 0:1]
        )

    fewer = pl.ds(0, side - 1)
    remote(row1.at[fewer], row1.at[fewer], sems.at[0], sems.at[1], partner).wait_recv()
    hops = []
    for i, peer in enumerate(second_peers):
        copy = remote(row1, row2.at[second_at], hop_sems.at[0, i], hop_sems.at[1, i], peer)
        copy.start()
        hops.append(copy)
    remote(row1, row3.at[second_at], sems.at[4], sems.at[5], partner).start()
    row2[pl.ds(second_at, 1)] = row1[...].reshape(1, side, coarse_count, width)
    remote(idx1.at[fewer], idx1.at[fewer], sems.at[2], sems.at[3], partner).wait_recv()
    for peer in second_peers:
        remote(idx1, idx2.at[second_at], sems.at[6], sems.at[7], peer).start()
    idx2[pl.ds(second_at, 1)] = idx1[...].reshape(1, side, 2, peers)

    proj[ext + own : send_pad, :] = jnp.zeros((send_pad - ext - own, width), BF16)
    proj[send_pad + own :, :] = jnp.zeros((recv_pad - own, width), BF16)
    dagg[own:, :] = jnp.zeros((recv_pad - own, width), BF16)
    copies[0].wait()
    proj[ext : ext + own, :] = mm(nodes[...], w_send[...]).astype(BF16)
    copies[1].wait()
    proj[send_pad : send_pad + own, :] = mm(nodes[...], w_recv[...]).astype(BF16)
    copies[2].wait()
    copies[3].wait()
    for copy in near:
        copy.wait_recv()
    proj[0:near_total, :] = mm(near_in[...].reshape(near_total, width), w_send[...]).astype(BF16)

    def ahead(step, carry):
        at = pl.ds(pl.multiple_of(step * rows, rows), rows)
        slope[at, :] = 0.5 * (
            mm(edges[at, :], w_edge[...])
            + mm(onehot[at, 0:near_total], proj[0:near_total, :])
            + mm(onehot[at, ext:], proj[ext:, :])
            + edge_bias[...]
        )
        return carry

    lax.fori_loop(0, steps, ahead, 0)

    for i in reversed(range(len(order))):
        hops[i].wait_recv()
        origin = wrapped(second_at + side - order[i], side)
        remote(row2.at[origin], row3.at[origin], sems.at[4], sems.at[5], partner).start()
    remote(idx2.at[fewer], idx2.at[fewer], sems.at[6], sems.at[7], partner).wait_recv()
    remote(idx2, idx3, sems.at[8], sems.at[9], partner).start()
    for i in (4, 5, 6, 7, 8):
        copies[i].wait()
    node_pre = mm(nodes[...], w_node[...]) + node_bias[...]
    node_back = node_cot[...].astype(F32)
    for w, turned in ((w_edge_out, w_edge_out_t), (w_node_out, w_node_out_t), (w_agg, w_agg_t), (w_send, w_send_t)):
        turned[...] = w[...].T
    live_rows = counts[0] * BLOCK

    half = area * coarse_count
    mine_rows = mm(picks[:, 0:half], row2[...].reshape(half, width))
    remote(row2, row3, sems.at[4], sems.at[5], partner).wait_recv()
    far_rows = mine_rows + mm(picks[:, half:], row3[...].reshape(half, width))
    proj[near_total:ext, :] = (0.5 * mm(far_rows.astype(BF16), w_send[...])).astype(BF16)

    gathered = []
    for step in range(steps):
        at = slice(step * rows, (step + 1) * rows)
        half_pre = slope[at, :] + mm(onehot[at, near_total:ext], proj[near_total:ext, :])
        hidden, rise = silu_both(half_pre)
        slope[at, :] = rise
        out = mm(hidden.astype(BF16), w_edge_out[...]) + edge_out_bias[...]
        center = out - jnp.mean(out, axis=-1, keepdims=True)
        inv = lax.rsqrt(jnp.mean(center * center, axis=-1, keepdims=True) + 1e-05)
        inv = jnp.where(iota((rows, 1), 0) + step * rows < live_rows, inv, 0.0)
        normed = center * inv
        unit[at, :] = normed
        invs[at, :] = jnp.broadcast_to(0.5 * inv, (rows, LANES))
        sent[at, :] = (edge_gain[...] * normed).astype(BF16)
        gathered.append(mm(onehot_t[send_pad : send_pad + own, at], sent[at, :]))

    nodes_back = []
    part = own // NODE_PARTS
    for h in range(NODE_PARTS):
        at = slice(h * part, (h + 1) * part)
        aggregate = sum(g[at] for g in gathered).astype(BF16)
        hidden, rise = silu_both(0.5 * (node_pre[at] + mm(aggregate, w_agg[...])))
        out = mm(hidden.astype(BF16), w_node_out[...]) + node_out_bias[...]
        normed, inv = normal_stats(out)
        new_nodes[at, :] = (nodes[at, :].astype(F32) + node_gain[...] * normed).astype(BF16)
        d_out = normal_back(node_gain[...] * node_back[at], normed, 0.5 * inv).astype(BF16)
        d_node = (mm(d_out, w_node_out_t[...]) * rise).astype(BF16)
        dagg[at, :] = mm(d_node, w_agg_t[...]).astype(BF16)
        nodes_back.append(d_node)
    d_node = jnp.concatenate(nodes_back, axis=0)

    gathered = []
    for step in range(steps):
        at = slice(step * rows, (step + 1) * rows)
        d_message = edge_cot[at, :].astype(F32) + mm(onehot[at, send_pad:], dagg[...])
        d_out = normal_back(edge_gain[...] * d_message, unit[at, :], invs[at, 0:1]).astype(BF16)
        dpre[at, :] = (mm(d_out, w_edge_out_t[...]) * slope[at, :]).astype(BF16)
        gathered.append(mm(onehot_t[0:ext, at], dpre[at, :]))

    sums = sum(gathered[1:], gathered[0]).astype(BF16)
    back = mm(sums, w_send_t[...])
    near_out_b[...] = back[0:near_total, :].astype(BF16).reshape(near_count, near_rows, width)
    pair = [back[near_total + s * peers : near_total + (s + 1) * peers, :] for s in range(2)]
    spread_rows(pair, wide, far_out_b, peers)
    near_b = []
    for k in range(near_count):
        copy = remote(
            near_out_b.at[k], near_in_b.at[k], near_send_b.at[k], near_recv_b.at[k],
            lax.rem(me - offsets[k] + peers, peers),
        )
        copy.start()
        near_b.append(copy)
    every_peer(
        me, side,
        lambda peer: remote(
            far_out_b.at[peer], far_in_b.at[me], sems.at[10], sems.at[11], peer
        ).start(),
    )
    far_in_b[pl.ds(me, 1)] = far_out_b[pl.ds(me, 1)]

    remote(idx2, idx3, sems.at[8], sems.at[9], partner).wait_recv()
    found = []
    for part in (idx2, idx3):
        listed = part[...].reshape(2 * area, peers)
        found.append(
            jnp.sum(jnp.where(iota(listed.shape, 1) == me, listed, 0), axis=1, keepdims=True)
        )
    found = jnp.concatenate(found, axis=0)
    slots_t = []
    for slot in range(2):
        there = iota((4 * area, peers), 0) == key * 2 + slot
        asked = jnp.sum(jnp.where(there, found, 0), axis=0, keepdims=True)
        line = jnp.zeros_like(asked)
        for c in range(coarse_count):
            line = jnp.where(asked == c, coarse[c], line)
        slots_t.append(line)
    sums = mm(onehot_t[ext : ext + own, :], dpre[...]).astype(BF16)
    total = node_back + mm_nt(d_node, w_node[...]) + mm(sums, w_send_t[...])
    sums = mm(onehot_t[send_pad : send_pad + own, :], dpre[...]).astype(BF16)
    total = total + mm_nt(sums, w_recv[...])

    def finish(step, carry):
        at = pl.ds(pl.multiple_of(step * rows, rows), rows)
        grad = edge_cot[at, :].astype(F32) + mm_nt(dpre[at, :], w_edge[...])
        edge_grad[at, :] = grad.astype(BF16)
        new_edges[at, :] = (edges[at, :].astype(F32) + edge_gain[...] * unit[at, :]).astype(BF16)
        return carry

    lax.fori_loop(0, steps, finish, 0)

    for k in range(near_count):
        near_b[k].wait_recv()
        mask = iota((own, near_rows), 0) == near_lists[k : k + 1, :]
        total = total + mm(hot(mask), near_in_b[k])
    remote(far_out_b.at[others], far_in_b.at[others], sems.at[10], sems.at[11], partner).wait_recv()
    pair = collect_rows(far_in_b, wide, peers, width)
    for s in range(2):
        mask = iota((own, peers), 0) == slots_t[s]
        total = total + mm(hot(mask), pair[s].astype(BF16))
    node_grad[...] = total.astype(BF16)
    for copy in near:
        copy.wait_send()
    for copy in near_b:
        copy.wait_send()
    remote(row1.at[fewer], row1.at[fewer], sems.at[0], sems.at[1], partner).wait_send()
    remote(idx1.at[fewer], idx1.at[fewer], sems.at[2], sems.at[3], partner).wait_send()
    for copy in hops:
        copy.wait_send()
    remote(row2, row3, sems.at[4], sems.at[5], partner).wait_send()
    remote(idx2.at[fewer], idx2.at[fewer], sems.at[6], sems.at[7], partner).wait_send()
    remote(idx2, idx3, sems.at[8], sems.at[9], partner).wait_send()
    remote(far_out_b.at[others], far_in_b.at[others], sems.at[10], sems.at[11], partner).wait_send()


def place_kernel(a, b, c, d, a_out, b_out, c_out, d_out, sems):
    pairs = ((b, b_out), (d, d_out), (a, a_out), (c, c_out))
    copies = [pltpu.make_async_copy(x, y, sems.at[i]) for i, (x, y) in enumerate(pairs)]
    for copy in copies:
        copy.start()
    for copy in copies:
        copy.wait()


VM = pl.BlockSpec(memory_space=pltpu.VMEM)
SM = pl.BlockSpec(memory_space=pltpu.SMEM)
HBM = pl.BlockSpec(memory_space=pltpu.HBM)
ANY = pl.BlockSpec(memory_space=pl.ANY)
DMA = pltpu.SemaphoreType.DMA
NODE_PARTS = 1


def local(
    nodes, edges, node_cot, edge_cot, w_edge, w_send, w_recv, edge_bias, w_edge_out,
    edge_out_bias, edge_gain, w_node, w_agg, node_bias, w_node_out, node_out_bias, node_gain,
    send_slots, recv_slots, neighbour_send_lists, coarse_rows, far_lists, block_count,
):
    own, width = nodes.shape
    total_edges = edges.shape[0]
    peers = lax.axis_size("patch")
    near_count, near_rows = neighbour_send_lists.shape
    near_total = near_count * near_rows
    ext = near_total + 2 * peers
    unit_rows = 2 * width // LANES
    send_pad = -(-(ext + own) // LANES) * LANES
    recv_pad = -(-own // LANES) * LANES
    flat = lambda v: v.reshape(1, -1)
    near_b = pltpu.VMEM((near_count, near_rows, width), BF16)
    side, coarse = side_of(peers), coarse_rows.shape[0]
    far_b = pltpu.VMEM((peers, unit_rows, LANES), BF16)
    node_b = pltpu.VMEM((own, width), BF16)
    slot_b = pltpu.VMEM((total_edges // LANES, LANES), jnp.int32)
    weight = pltpu.VMEM((width, width), BF16)
    edge_b = pltpu.VMEM((total_edges, width), BF16)
    edge_f = pltpu.VMEM((total_edges, width), F32)
    shapes = tuple(
        jax.ShapeDtypeStruct((n, width), BF16) for n in (own, total_edges, own, total_edges)
    )
    results = pl.pallas_call(
        functools.partial(layer_kernel, total_edges, peers),
        name="layer",
        out_shape=tuple(pltpu.VMEM(v.shape, v.dtype) for v in shapes),
        in_specs=[SM] + [HBM] * 22,
        out_specs=(VM,) * 4,
        scratch_shapes=[near_b] * 4
        + [pltpu.VMEM((peers * unit_rows, LANES), F32)] + [far_b] * 2
        + [
            pltpu.VMEM((side, coarse, width), BF16),
            pltpu.VMEM((side, side, coarse, width), BF16),
            pltpu.VMEM((side, side, coarse, width), BF16),
            pltpu.VMEM((side, 2, peers), jnp.int32),
            pltpu.VMEM((side, side, 2, peers), jnp.int32),
            pltpu.VMEM((side, side, 2, peers), jnp.int32),
            pltpu.VMEM((2 * peers, 2 * side * side * coarse), BF16),
        ]
        + [
            node_b, pltpu.VMEM(neighbour_send_lists.shape, jnp.int32), pltpu.VMEM((1, 2, peers), jnp.int32),
            pltpu.SMEM(coarse_rows.shape, jnp.int32), slot_b, slot_b, node_b,
        ]
        + [pltpu.VMEM((1, width), F32)] * 6
        + [edge_b] * 2 + [weight] * 11
        + [
            pltpu.VMEM((send_pad + recv_pad, width), BF16),
            pltpu.VMEM((total_edges, send_pad + recv_pad), BF16),
            pltpu.VMEM((send_pad + recv_pad, total_edges), BF16),
            edge_f, edge_f,
            pltpu.VMEM((total_edges, LANES), F32),
            edge_b, edge_b,
            pltpu.VMEM((recv_pad, width), BF16),
        ]
        + [DMA((near_count,))] * 4 + [DMA((12,)), DMA((2, side - 1)), DMA((22,))],
        compiler_params=pltpu.CompilerParams(
            collective_id=0, has_side_effects=True, vmem_limit_bytes=VMEM_LIMIT
        ),
    )(
        block_count, nodes, neighbour_send_lists, far_lists.transpose(0, 2, 1), coarse_rows,
        send_slots.reshape(-1, LANES), recv_slots.reshape(-1, LANES), node_cot,
        flat(edge_bias), flat(edge_out_bias), flat(edge_gain), flat(node_bias),
        flat(node_out_bias), flat(node_gain),
        edges, edge_cot, w_edge, w_send, w_recv, w_edge_out, w_node, w_agg, w_node_out,
    )
    return pl.pallas_call(
        place_kernel,
        name="place",
        out_shape=shapes,
        in_specs=[VM] * 4,
        out_specs=(ANY,) * 4,
        scratch_shapes=[DMA((4,))],
        compiler_params=pltpu.CompilerParams(vmem_limit_bytes=8 << 20),
    )(*results)


def solution(mesh):
    both = P(("groups", "patch"), None)
    placed = (both,) * 4 + (P(),) * 13 + (
        P("patch"), P("patch"), P("patch", None), P("patch"), P("patch", None, None), P("patch"),
    )
    return jax.shard_map(
        local, mesh=mesh, in_specs=placed, out_specs=(both,) * 4, check_vma=False
    )
```

```python
import functools
import math

import jax
import jax.numpy as jnp
from jax import lax
from jax.experimental import pallas as pl
from jax.experimental.pallas import tpu as pltpu
from jax.sharding import PartitionSpec as P

BLOCK = 128
LANES = 128
MESH = pl.DeviceIdType.MESH
F32 = jnp.float32
BF16 = jnp.bfloat16
VMEM_LIMIT = 60 << 20


def mm(a, b):
    return lax.dot_general(a, b, (((1,), (0,)), ((), ())), preferred_element_type=F32)


def mm_nt(a, b):
    return lax.dot_general(a, b, (((1,), (1,)), ((), ())), preferred_element_type=F32)


def mm_tn(a, b):
    return lax.dot_general(a, b, (((0,), (0,)), ((), ())), preferred_element_type=F32)


def iota(shape, dim):
    return lax.broadcasted_iota(jnp.int32, shape, dim)


def hot(mask):
    return jnp.where(mask, 1.0, 0.0).astype(BF16)


def offsets_of(count):
    return [(index // 2 + 1) * (1 - 2 * (index % 2)) for index in range(count)]


def side_of(peers):
    return math.isqrt(peers // 2)


def far_first(side):
    half = side // 2
    return sorted(range(1, side), key=lambda k: -min(k, side - k)) if half else []


def place_of(me, side):
    core = lax.rem(me, 2)
    line = lax.rem(lax.div(me, 2), side)
    return lax.div(me, 2 * side), line, core


def wrapped(value, side):
    return jnp.where(value >= side, value - side, value)


def every_peer(me, side, body):
    x, y, core = place_of(me, side)
    within = [(oy, oc) for oy in far_first(side) + [0] for oc in (0, 1)]
    lines = {oy: 2 * wrapped(y + oy, side) for oy in range(side)}
    cores = (core, 1 - core)

    def step(i, carry):
        away = lax.div(i + 1, 2) * (1 - 2 * lax.rem(i, 2))
        row = wrapped(x + side // 2 + away, side) * (2 * side)
        for oy, oc in within:
            body(row + lines[oy] + cores[oc])
        return carry

    lax.fori_loop(0, side - 1, step, 0)
    for oy, oc in within[:-2] + [(0, 1)]:
        body(x * (2 * side) + lines[oy] + cores[oc])


def remote(src, dst, send, recv, peer):
    return pltpu.make_async_remote_copy(
        src_ref=src, dst_ref=dst, send_sem=send, recv_sem=recv,
        device_id={"patch": peer}, device_id_type=MESH,
    )


def spread_rows(pair, wide, packed, peers):
    parts = pair[0].shape[1] // LANES
    unit = 2 * parts
    for slot in range(2):
        for part in range(parts):
            wide[pl.ds(2 * part + slot, peers, stride=unit), :] = pair[slot][
                :, part * LANES : (part + 1) * LANES
            ]
    packed[...] = wide[...].reshape(peers, unit, LANES).astype(BF16)


def collect_rows(packed, wide, peers, width):
    parts = width // LANES
    unit = 2 * parts
    wide[...] = packed[...].astype(F32).reshape(peers * unit, LANES)
    pair = []
    for slot in range(2):
        pieces = [
            wide[pl.ds(2 * part + slot, peers, stride=unit), :] for part in range(parts)
        ]
        pair.append(jnp.concatenate(pieces, axis=1))
    return pair


def normal_stats(values):
    center = values - jnp.mean(values, axis=-1, keepdims=True)
    spread = jnp.mean(center * center, axis=-1, keepdims=True)
    inv = lax.rsqrt(spread + 1e-05)
    return center * inv, inv


def normal_back(grad, unit, inv):
    along = jnp.mean(grad * unit, axis=-1, keepdims=True)
    return inv * (grad - jnp.mean(grad, axis=-1, keepdims=True) - unit * along)


def silu_both(half):
    t = jnp.tanh(half)
    out = half + half * t
    return out, (1.0 + t) + out * (1.0 - t)


def layer_kernel(
    rows, peers,
    counts,
    nodes_h, near_lists_h, far_lists_h, coarse_h, send_rows_h, recv_rows_h, node_cot_h,
    edge_bias_h, edge_out_bias_h, edge_gain_h, node_bias_h, node_out_bias_h, node_gain_h,
    edges_h, edge_cot_h, w_edge_h, w_send_h, w_recv_h, w_edge_out_h, w_node_h, w_agg_h, w_node_out_h,
    new_nodes, new_edges, node_grad, edge_grad,
    near_out, near_in, near_out_b, near_in_b, wide, far_out_b, far_in_b,
    row1, row2, row3, idx1, idx2, idx3, picks,
    nodes, near_lists, far_lists, coarse, send_rows, recv_rows, node_cot,
    edge_bias, edge_out_bias, edge_gain, node_bias, node_out_bias, node_gain,
    edges, edge_cot, w_edge, w_send, w_recv, w_edge_out, w_node, w_agg, w_node_out,
    w_edge_out_t, w_node_out_t, w_agg_t, w_send_t,
    proj, onehot, onehot_t, slope, unit, invs, sent, dpre, dagg,
    near_send, near_recv, near_send_b, near_recv_b, sems, hop_sems, in_sems,
):
    me = lax.axis_index("patch")
    own, width = nodes.shape
    total_edges = edges.shape[0]
    near_count, near_rows = near_lists.shape
    near_total = near_count * near_rows
    ext = near_total + 2 * peers
    send_pad = -(-(ext + own) // LANES) * LANES
    recv_pad = -(-own // LANES) * LANES
    steps = total_edges // rows
    offsets = offsets_of(near_count)
    others = pl.ds(0, peers - 1)

    side = side_of(peers)
    x, y, core = place_of(me, side)
    first_step = jnp.where(core == 0, 2 * side, 2)
    second_step = jnp.where(core == 0, 2, 2 * side)
    first_at = jnp.where(core == 0, x, y)
    second_at = jnp.where(core == 0, y, x)
    partner = me + 1 - 2 * core
    order = far_first(side)
    first_peers = [me + (wrapped(first_at + k, side) - first_at) * first_step for k in order]
    second_peers = [me + (wrapped(second_at + k, side) - second_at) * second_step for k in order]
    near_peers = [lax.rem(me + o + peers, peers) for o in offsets]
    barrier = pltpu.get_barrier_semaphore()
    known = first_peers + second_peers + near_peers + [partner]
    for peer in known:
        pl.semaphore_signal(barrier, inc=1, device_id={"patch": peer}, device_id_type=MESH)
    moves = [
        (nodes_h, nodes), (near_lists_h, near_lists), (far_lists_h, far_lists), (coarse_h, coarse),
        (send_rows_h, send_rows), (recv_rows_h, recv_rows), (edge_bias_h, edge_bias),
        (edge_out_bias_h, edge_out_bias), (edge_gain_h, edge_gain), (node_bias_h, node_bias),
        (node_out_bias_h, node_out_bias), (node_gain_h, node_gain), (node_cot_h, node_cot),
        (w_send_h, w_send), (w_recv_h, w_recv), (edges_h, edges), (w_edge_h, w_edge),
        (w_edge_out_h, w_edge_out), (w_agg_h, w_agg), (w_node_h, w_node),
        (w_node_out_h, w_node_out), (edge_cot_h, edge_cot),
    ]
    copies = [pltpu.make_async_copy(a, b, in_sems.at[i]) for i, (a, b) in enumerate(moves)]
    first_big = len(copies) - 9
    for copy in copies[:4]:
        copy.start()

    for i in range(4):
        copies[i].wait()
    coarse_count = coarse.shape[0]
    chosen = jnp.zeros((coarse_count, own), jnp.int32)
    for c in range(coarse_count):
        chosen = jnp.where(iota(chosen.shape, 0) == c, coarse[c], chosen)
    rows_out = mm(hot(iota(chosen.shape, 1) == chosen), nodes[...]).astype(BF16)
    row1[pl.ds(first_at, 1)] = rows_out.reshape(1, coarse_count, width)
    idx1[pl.ds(first_at, 1)] = far_lists[...]

    pl.semaphore_wait(barrier, len(known))
    mine = row1.at[first_at]
    for peer in first_peers:
        remote(mine, mine, sems.at[0], sems.at[1], peer).start()
    for copy in copies[4:]:
        copy.start()
    for k in range(near_count):
        mask = iota((own, near_rows), 0) == near_lists[k : k + 1, :]
        near_out[k] = mm_tn(hot(mask), nodes[...]).astype(BF16)
    near = []
    for k in range(near_count):
        copy = remote(near_out.at[k], near_in.at[k], near_send.at[k], near_recv.at[k], near_peers[k])
        copy.start()
        near.append(copy)
    mine = idx1.at[first_at]
    for peer in first_peers:
        remote(mine, mine, sems.at[2], sems.at[3], peer).start()

    for i in range(4, first_big):
        copies[i].wait()
    copies = copies[first_big:]
    raw = send_rows[...]
    far = raw - own - near_total
    address = jnp.where(
        raw < own, raw + ext,
        jnp.where(raw < own + near_total, raw - own,
                  near_total + jnp.bitwise_and(far, 1) * peers + lax.shift_right_arithmetic(far, 1)),
    )
    target = recv_rows[...]
    lane = iota((LANES, LANES), 1)
    for g in range(total_edges // LANES):
        line = address[g : g + 1, :]
        goal = target[g : g + 1, :]
        span = slice(g * LANES, (g + 1) * LANES)
        onehot_t[0:send_pad, span] = hot(iota((send_pad, LANES), 0) == line)
        onehot_t[send_pad:, span] = hot(iota((recv_pad, LANES), 0) == goal)
        line_col = jnp.broadcast_to(line, (LANES, LANES)).T
        goal_col = jnp.broadcast_to(goal, (LANES, LANES)).T
        for c in range(send_pad // LANES):
            onehot[span, c * LANES : (c + 1) * LANES] = hot(line_col == lane + c * LANES)
        for c in range(recv_pad // LANES):
            onehot[span, send_pad + c * LANES : send_pad + (c + 1) * LANES] = hot(
                goal_col == lane + c * LANES
            )
    area = side * side
    q = iota((1, peers), 1)
    q_core = jnp.bitwise_and(q, 1)
    q_chip = lax.shift_right_logical(q, 1)
    q_x = q_chip // side
    q_y = q_chip - q_x * side
    key = jnp.where(q_core == 0, q_y * side + q_x, q_x * side + q_y)
    key = key + jnp.where(q_core == core, 0, area)
    for slot in range(2):
        spot = key * coarse_count + far_lists[0, slot : slot + 1, :]
        spot_col = jnp.broadcast_to(spot, (LANES, peers)).T
        picks[slot * peers : (slot + 1) * peers, :] = hot(
            iota((peers, 2 * area * coarse_count), 1) == spot_col[:, 0:1]
        )

    fewer = pl.ds(0, side - 1)
    remote(row1.at[fewer], row1.at[fewer], sems.at[0], sems.at[1], partner).wait_recv()
    hops = []
    for i, peer in enumerate(second_peers):
        copy = remote(row1, row2.at[second_at], hop_sems.at[0, i], hop_sems.at[1, i], peer)
        copy.start()
        hops.append(copy)
    remote(row1, row3.at[second_at], sems.at[4], sems.at[5], partner).start()
    row2[pl.ds(second_at, 1)] = row1[...].reshape(1, side, coarse_count, width)
    remote(idx1.at[fewer], idx1.at[fewer], sems.at[2], sems.at[3], partner).wait_recv()
    for peer in second_peers:
        remote(idx1, idx2.at[second_at], sems.at[6], sems.at[7], peer).start()
    idx2[pl.ds(second_at, 1)] = idx1[...].reshape(1, side, 2, peers)

    proj[ext + own : send_pad, :] = jnp.zeros((send_pad - ext - own, width), BF16)
    proj[send_pad + own :, :] = jnp.zeros((recv_pad - own, width), BF16)
    dagg[own:, :] = jnp.zeros((recv_pad - own, width), BF16)
    copies[0].wait()
    proj[ext : ext + own, :] = mm(nodes[...], w_send[...]).astype(BF16)
    copies[1].wait()
    proj[send_pad : send_pad + own, :] = mm(nodes[...], w_recv[...]).astype(BF16)
    copies[2].wait()
    copies[3].wait()
    for copy in near:
        copy.wait_recv()
    proj[0:near_total, :] = mm(near_in[...].reshape(near_total, width), w_send[...]).astype(BF16)

    def ahead(step, carry):
        at = pl.ds(pl.multiple_of(step * rows, rows), rows)
        slope[at, :] = 0.5 * (
            mm(edges[at, :], w_edge[...])
            + mm(onehot[at, 0:near_total], proj[0:near_total, :])
            + mm(onehot[at, ext:], proj[ext:, :])
            + edge_bias[...]
        )
        return carry

    lax.fori_loop(0, steps, ahead, 0)

    for i in reversed(range(len(order))):
        hops[i].wait_recv()
        origin = wrapped(second_at + side - order[i], side)
        remote(row2.at[origin], row3.at[origin], sems.at[4], sems.at[5], partner).start()
    remote(idx2.at[fewer], idx2.at[fewer], sems.at[6], sems.at[7], partner).wait_recv()
    remote(idx2, idx3, sems.at[8], sems.at[9], partner).start()
    for i in (4, 5, 6, 7, 8):
        copies[i].wait()
    node_pre = mm(nodes[...], w_node[...]) + node_bias[...]
    node_back = node_cot[...].astype(F32)
    for w, turned in ((w_edge_out, w_edge_out_t), (w_node_out, w_node_out_t), (w_agg, w_agg_t), (w_send, w_send_t)):
        turned[...] = w[...].T
    live_rows = counts[0] * BLOCK

    half = area * coarse_count
    mine_rows = mm(picks[:, 0:half], row2[...].reshape(half, width))
    remote(row2, row3, sems.at[4], sems.at[5], partner).wait_recv()
    far_rows = mine_rows + mm(picks[:, half:], row3[...].reshape(half, width))
    proj[near_total:ext, :] = (0.5 * mm(far_rows.astype(BF16), w_send[...])).astype(BF16)

    gathered = []
    for step in range(steps):
        at = slice(step * rows, (step + 1) * rows)
        half_pre = slope[at, :] + mm(onehot[at, near_total:ext], proj[near_total:ext, :])
        hidden, rise = silu_both(half_pre)
        slope[at, :] = rise
        out = mm(hidden.astype(BF16), w_edge_out[...]) + edge_out_bias[...]
        center = out - jnp.mean(out, axis=-1, keepdims=True)
        inv = lax.rsqrt(jnp.mean(center * center, axis=-1, keepdims=True) + 1e-05)
        inv = jnp.where(iota((rows, 1), 0) + step * rows < live_rows, inv, 0.0)
        normed = center * inv
        unit[at, :] = normed
        invs[at, :] = jnp.broadcast_to(0.5 * inv, (rows, LANES))
        sent[at, :] = (edge_gain[...] * normed).astype(BF16)
        gathered.append(mm(onehot_t[send_pad : send_pad + own, at], sent[at, :]))

    nodes_back = []
    part = own // NODE_PARTS
    for h in range(NODE_PARTS):
        at = slice(h * part, (h + 1) * part)
        aggregate = sum(g[at] for g in gathered).astype(BF16)
        hidden, rise = silu_both(0.5 * (node_pre[at] + mm(aggregate, w_agg[...])))
        out = mm(hidden.astype(BF16), w_node_out[...]) + node_out_bias[...]
        normed, inv = normal_stats(out)
        new_nodes[at, :] = (nodes[at, :].astype(F32) + node_gain[...] * normed).astype(BF16)
        d_out = normal_back(node_gain[...] * node_back[at], normed, 0.5 * inv).astype(BF16)
        d_node = (mm(d_out, w_node_out_t[...]) * rise).astype(BF16)
        dagg[at, :] = mm(d_node, w_agg_t[...]).astype(BF16)
        nodes_back.append(d_node)
    d_node = jnp.concatenate(nodes_back, axis=0)

    gathered = []
    for step in range(steps):
        at = slice(step * rows, (step + 1) * rows)
        d_message = edge_cot[at, :].astype(F32) + mm(onehot[at, send_pad:], dagg[...])
        d_out = normal_back(edge_gain[...] * d_message, unit[at, :], invs[at, 0:1]).astype(BF16)
        dpre[at, :] = (mm(d_out, w_edge_out_t[...]) * slope[at, :]).astype(BF16)
        gathered.append(mm(onehot_t[0:ext, at], dpre[at, :]))

    sums = sum(gathered[1:], gathered[0]).astype(BF16)
    back = mm(sums, w_send_t[...])
    near_out_b[...] = back[0:near_total, :].astype(BF16).reshape(near_count, near_rows, width)
    pair = [back[near_total + s * peers : near_total + (s + 1) * peers, :] for s in range(2)]
    spread_rows(pair, wide, far_out_b, peers)
    every_peer(
        me, side,
        lambda peer: remote(
            far_out_b.at[peer], far_in_b.at[me], sems.at[10], sems.at[11], peer
        ).start(),
    )
    near_b = []
    for k in range(near_count):
        copy = remote(
            near_out_b.at[k], near_in_b.at[k], near_send_b.at[k], near_recv_b.at[k],
            lax.rem(me - offsets[k] + peers, peers),
        )
        copy.start()
        near_b.append(copy)
    far_in_b[pl.ds(me, 1)] = far_out_b[pl.ds(me, 1)]

    remote(idx2, idx3, sems.at[8], sems.at[9], partner).wait_recv()
    found = []
    for part in (idx2, idx3):
        listed = part[...].reshape(2 * area, peers)
        found.append(
            jnp.sum(jnp.where(iota(listed.shape, 1) == me, listed, 0), axis=1, keepdims=True)
        )
    found = jnp.concatenate(found, axis=0)
    slots_t = []
    for slot in range(2):
        there = iota((4 * area, peers), 0) == key * 2 + slot
        asked = jnp.sum(jnp.where(there, found, 0), axis=0, keepdims=True)
        line = jnp.zeros_like(asked)
        for c in range(coarse_count):
            line = jnp.where(asked == c, coarse[c], line)
        slots_t.append(line)
    sums = mm(onehot_t[ext : ext + own, :], dpre[...]).astype(BF16)
    total = node_back + mm_nt(d_node, w_node[...]) + mm(sums, w_send_t[...])
    sums = mm(onehot_t[send_pad : send_pad + own, :], dpre[...]).astype(BF16)
    total = total + mm_nt(sums, w_recv[...])

    def finish(step, carry):
        at = pl.ds(pl.multiple_of(step * rows, rows), rows)
        grad = edge_cot[at, :].astype(F32) + mm_nt(dpre[at, :], w_edge[...])
        edge_grad[at, :] = grad.astype(BF16)
        new_edges[at, :] = (edges[at, :].astype(F32) + edge_gain[...] * unit[at, :]).astype(BF16)
        return carry

    lax.fori_loop(0, steps, finish, 0)

    near_masks = [
        hot(iota((own, near_rows), 0) == near_lists[k : k + 1, :]) for k in range(near_count)
    ]
    far_masks = [hot(iota((own, peers), 0) == slots_t[s]) for s in range(2)]
    for k in range(near_count):
        near_b[k].wait_recv()
        total = total + mm(near_masks[k], near_in_b[k])
    remote(far_out_b.at[others], far_in_b.at[others], sems.at[10], sems.at[11], partner).wait_recv()
    pair = collect_rows(far_in_b, wide, peers, width)
    for s in range(2):
        total = total + mm(far_masks[s], pair[s].astype(BF16))
    node_grad[...] = total.astype(BF16)
    for copy in near:
        copy.wait_send()
    for copy in near_b:
        copy.wait_send()
    remote(row1.at[fewer], row1.at[fewer], sems.at[0], sems.at[1], partner).wait_send()
    remote(idx1.at[fewer], idx1.at[fewer], sems.at[2], sems.at[3], partner).wait_send()
    for copy in hops:
        copy.wait_send()
    remote(row2, row3, sems.at[4], sems.at[5], partner).wait_send()
    remote(idx2.at[fewer], idx2.at[fewer], sems.at[6], sems.at[7], partner).wait_send()
    remote(idx2, idx3, sems.at[8], sems.at[9], partner).wait_send()
    remote(far_out_b.at[others], far_in_b.at[others], sems.at[10], sems.at[11], partner).wait_send()


PIECES = 4


def place_kernel(a, b, c, d, a_out, b_out, c_out, d_out, sems):
    copies = []
    for x, y in ((b, b_out), (d, d_out)):
        rows = x.shape[0] // PIECES
        for i in range(PIECES):
            at = pl.ds(i * rows, rows)
            copies.append(pltpu.make_async_copy(x.at[at], y.at[at], sems.at[len(copies)]))
    for x, y in ((a, a_out), (c, c_out)):
        copies.append(pltpu.make_async_copy(x, y, sems.at[len(copies)]))
    for copy in copies:
        copy.start()
    for copy in copies:
        copy.wait()


VM = pl.BlockSpec(memory_space=pltpu.VMEM)
SM = pl.BlockSpec(memory_space=pltpu.SMEM)
HBM = pl.BlockSpec(memory_space=pltpu.HBM)
ANY = pl.BlockSpec(memory_space=pl.ANY)
DMA = pltpu.SemaphoreType.DMA
NODE_PARTS = 1


def local(
    nodes, edges, node_cot, edge_cot, w_edge, w_send, w_recv, edge_bias, w_edge_out,
    edge_out_bias, edge_gain, w_node, w_agg, node_bias, w_node_out, node_out_bias, node_gain,
    send_slots, recv_slots, neighbour_send_lists, coarse_rows, far_lists, block_count,
):
    own, width = nodes.shape
    total_edges = edges.shape[0]
    peers = lax.axis_size("patch")
    near_count, near_rows = neighbour_send_lists.shape
    near_total = near_count * near_rows
    ext = near_total + 2 * peers
    unit_rows = 2 * width // LANES
    send_pad = -(-(ext + own) // LANES) * LANES
    recv_pad = -(-own // LANES) * LANES
    flat = lambda v: v.reshape(1, -1)
    near_b = pltpu.VMEM((near_count, near_rows, width), BF16)
    side, coarse = side_of(peers), coarse_rows.shape[0]
    far_b = pltpu.VMEM((peers, unit_rows, LANES), BF16)
    node_b = pltpu.VMEM((own, width), BF16)
    slot_b = pltpu.VMEM((total_edges // LANES, LANES), jnp.int32)
    weight = pltpu.VMEM((width, width), BF16)
    edge_b = pltpu.VMEM((total_edges, width), BF16)
    edge_f = pltpu.VMEM((total_edges, width), F32)
    shapes = tuple(
        jax.ShapeDtypeStruct((n, width), BF16) for n in (own, total_edges, own, total_edges)
    )
    results = pl.pallas_call(
        functools.partial(layer_kernel, total_edges, peers),
        name="layer",
        out_shape=tuple(pltpu.VMEM(v.shape, v.dtype) for v in shapes),
        in_specs=[SM] + [HBM] * 22,
        out_specs=(VM,) * 4,
        scratch_shapes=[near_b] * 4
        + [pltpu.VMEM((peers * unit_rows, LANES), F32)] + [far_b] * 2
        + [
            pltpu.VMEM((side, coarse, width), BF16),
            pltpu.VMEM((side, side, coarse, width), BF16),
            pltpu.VMEM((side, side, coarse, width), BF16),
            pltpu.VMEM((side, 2, peers), jnp.int32),
            pltpu.VMEM((side, side, 2, peers), jnp.int32),
            pltpu.VMEM((side, side, 2, peers), jnp.int32),
            pltpu.VMEM((2 * peers, 2 * side * side * coarse), BF16),
        ]
        + [
            node_b, pltpu.VMEM(neighbour_send_lists.shape, jnp.int32), pltpu.VMEM((1, 2, peers), jnp.int32),
            pltpu.SMEM(coarse_rows.shape, jnp.int32), slot_b, slot_b, node_b,
        ]
        + [pltpu.VMEM((1, width), F32)] * 6
        + [edge_b] * 2 + [weight] * 11
        + [
            pltpu.VMEM((send_pad + recv_pad, width), BF16),
            pltpu.VMEM((total_edges, send_pad + recv_pad), BF16),
            pltpu.VMEM((send_pad + recv_pad, total_edges), BF16),
            edge_f, edge_f,
            pltpu.VMEM((total_edges, LANES), F32),
            edge_b, edge_b,
            pltpu.VMEM((recv_pad, width), BF16),
        ]
        + [DMA((near_count,))] * 4 + [DMA((12,)), DMA((2, side - 1)), DMA((22,))],
        compiler_params=pltpu.CompilerParams(
            collective_id=0, has_side_effects=True, vmem_limit_bytes=VMEM_LIMIT
        ),
    )(
        block_count, nodes, neighbour_send_lists, far_lists.transpose(0, 2, 1), coarse_rows,
        send_slots.reshape(-1, LANES), recv_slots.reshape(-1, LANES), node_cot,
        flat(edge_bias), flat(edge_out_bias), flat(edge_gain), flat(node_bias),
        flat(node_out_bias), flat(node_gain),
        edges, edge_cot, w_edge, w_send, w_recv, w_edge_out, w_node, w_agg, w_node_out,
    )
    return pl.pallas_call(
        place_kernel,
        name="place",
        out_shape=shapes,
        in_specs=[VM] * 4,
        out_specs=(ANY,) * 4,
        scratch_shapes=[DMA((2 * PIECES + 2,))],
        compiler_params=pltpu.CompilerParams(vmem_limit_bytes=8 << 20),
    )(*results)


def solution(mesh):
    both = P(("groups", "patch"), None)
    placed = (both,) * 4 + (P(),) * 13 + (
        P("patch"), P("patch"), P("patch", None), P("patch"), P("patch", None, None), P("patch"),
    )
    return jax.shard_map(
        local, mesh=mesh, in_specs=placed, out_specs=(both,) * 4, check_vma=False
    )
```
